256 devices in a mesh: gz: 32 (over z, x_hi, core), vert: 8 (over y, x_lo).
Axes of the slice: x: 4 (x_hi: 2, x_lo: 2; x = x_hi * 2 + x_lo), y: 4, z: 8, core: 2. Of those that a mesh axis runs over, the one named last changes fastest.
Arguments:
- volume: float32 [256, 128, 1024], P('gz'), may hold values from -6 to 6
- angle_index: int32 [32], P('vert'), may hold values from 0 to 511
- detector_rows: int32 [128], replicated, may hold values from 0 to 127, each once
- measured: float32 [32, 128, 1024], P('vert', 'gz'), may hold values from -96 to 96
Outputs:
- residual: float32 [32, 128, 1024], P('vert', 'gz')
- gradient: float32 [256, 128, 1024], P('gz', 'vert')
The draws below stay inside these ranges and needn't reach their ends.
All inputs are finite; a program needn't handle non-finite values.
Results may differ from the reference program's by a relative error of at most 0.0003.
Values sent between devices are 32-bit elements; how exact they have to be, the bound alone decides.
No kernel may reach another device: no remote copies, remote signals or barrier semaphores. Data moves between devices by JAX's collectives and lax.ppermute only.
A program may use at most 64 MiB of HBM per device.

```python
import jax
import jax.numpy as jnp
from jax import lax

X = 1024
ANGLES = 512
NZ = 256
Y = 128
VIEWS = 32


def touch_ends(result, own_key, least, top_value):
    longest = result.shape.index(max(result.shape))
    spots = []
    for shift in (0, 1):
        where = [jax.random.randint(jax.random.fold_in(own_key, axis), (), 0, length) for axis, length in enumerate(result.shape)]
        where[longest] = (where[longest] + shift) % result.shape[longest]
        spots.append(tuple(where))
    return result.at[spots[0]].set(least).at[spots[1]].set(top_value)


def block_levels(rng, extent, pieces, least, high):
    loudness, own = 1.0, jax.random.fold_in(rng, 6)
    for axis_at, shards_of in pieces:
        heights = jnp.exp(jax.random.uniform(jax.random.fold_in(own, axis_at), (shards_of,), jnp.float32, least / len(pieces), high / len(pieces)))
        loudness = loudness * jnp.repeat(heights, extent[axis_at] // shards_of).reshape([-1 if axis == axis_at else 1 for axis in range(len(extent))])
    return loudness


def noise(key, dims, scale, reach, shards=(), kind=jnp.bfloat16):
    result = jax.random.normal(key, dims, jnp.float32) * scale
    if len(shards) > 0:
        result = block_levels(key, dims, shards, -0.22, 0.18) * result
    return jnp.clip(result, min=-reach, max=reach).astype(kind)


def setup_inputs(seed: int = 0) -> dict:
    streams_of = jax.random.split(jax.random.key(seed), 5)
    volume = noise(streams_of[0], (NZ, Y, X), 1.0, 6.0, ((0, 32),), jnp.float32)
    angle_index = touch_ends(jax.random.randint(streams_of[1], (VIEWS,), 0, ANGLES), jax.random.fold_in(streams_of[1], 1), 0, ANGLES - 1).astype(jnp.int32)
    detector_rows = jax.random.permutation(streams_of[2], Y).astype(jnp.int32)
    measured = noise(streams_of[3], (VIEWS, Y, X), 16.0, 96.0, ((0, 8), (1, 32)), jnp.float32)
    return {"volume": volume, "angle_index": angle_index, "detector_rows": detector_rows, "measured": measured}


def shifts(depth_pos, angle_value):
    slope_num = 2 * angle_value - ANGLES
    product = depth_pos * slope_num
    shift_whole = jnp.floor_divide(product, ANGLES)
    shift_part = (product - shift_whole * ANGLES).astype(jnp.float32) / ANGLES
    slope_value = slope_num.astype(jnp.float32) / ANGLES
    weight = jnp.sqrt(1.0 + slope_value * slope_value)
    return (shift_whole.astype(jnp.int32), shift_part, weight)

def reference(volume, angle_index, detector_rows, measured):
    margin = NZ // 2 + 2
    padded = jnp.pad(volume, ((0, 0), (0, 0), (margin, margin)))
    depth_pos = jnp.arange(NZ, dtype=jnp.int32) - NZ // 2

    def project(angle_value):
        shift_whole, shift_part, weight = shifts(depth_pos, angle_value)

        def shifted(plane, offset, fraction):
            window = lax.dynamic_slice_in_dim(plane, offset, X + 1, 1)
            return (1.0 - fraction) * window[:, :-1] + fraction * window[:, 1:]
        contrib = jax.vmap(shifted)(padded, margin + shift_whole, shift_part)
        return weight * lax.optimization_barrier(jnp.sum(contrib, axis=0))
    projection = lax.map(project, angle_index)
    det_order = jnp.take(projection, detector_rows, axis=1)
    residual = (det_order - measured) * NZ ** (-0.5)
    back = jnp.zeros_like(residual).at[:, detector_rows, :].set(residual)
    back_pad = jnp.pad(back, ((0, 0), (0, 0), (margin, margin)))

    def add_view(running, view_item):
        plane, angle_value = view_item
        shift_whole, shift_part, weight = shifts(depth_pos, angle_value)

        def shifted(offset, fraction):
            window = lax.dynamic_slice_in_dim(plane, offset, X + 1, 1)
            return (1.0 - fraction) * window[:, 1:] + fraction * window[:, :-1]
        contrib = jax.vmap(shifted)(margin - shift_whole - 1, shift_part)
        return (running + weight * contrib, None)
    start_sum = jnp.zeros((NZ, Y, X), jnp.float32)
    summed, _ = lax.scan(add_view, start_sum, (back_pad, angle_index))
    gradient = summed * VIEWS ** (-0.5)
    return (residual, gradient)
```

```python
import functools

import jax
import jax.numpy as jnp
from jax import lax
from jax.experimental import pallas as pl
from jax.experimental.pallas import tpu as pltpu
from jax.sharding import PartitionSpec as P

ANGLES = 512
LANES = 128
VMEM = pltpu.VMEM
SMEM = pltpu.SMEM


def take_rows_kernel(rows_ref, half_ref, slab_ref, out_ref):
    peers = out_ref.shape[0]
    chunks = out_ref.shape[2]
    place = lax.broadcasted_iota(jnp.int32, (chunks, LANES), 0)

    def one(peer, carry):
        row = rows_ref[peer]
        start = pl.multiple_of(row // 8 * 8, 8)
        inside = row - start
        found = None
        for chunk in range(chunks):
            tile = slab_ref[0, pl.ds(start, 8), pl.ds(chunk * LANES, LANES)]
            turned = pltpu.roll(tile, (chunk + 8 - inside) % 8, 0)
            found = turned if found is None else jnp.where(place == chunk, turned, found)
        out_ref[peer, 0] = found
        return carry

    lax.fori_loop(0, peers, one, 0, unroll=4)


def take_rows(volume, rows, half):
    layers, row_count, columns = volume.shape
    peers = rows.shape[0]
    part = layers // 2
    chunks = columns // LANES
    return pl.pallas_call(
        take_rows_kernel,
        grid_spec=pltpu.PrefetchScalarGridSpec(
            num_scalar_prefetch=2,
            grid=(part,),
            in_specs=[
                pl.BlockSpec(
                    (1, row_count, columns),
                    lambda layer, rows_ref, half_ref: (half_ref[0] * part + layer, 0, 0),
                )
            ],
            out_specs=pl.BlockSpec(
                (peers, 1, chunks, LANES), lambda layer, rows_ref, half_ref: (0, layer, 0, 0)
            ),
        ),
        out_shape=jax.ShapeDtypeStruct((peers, part, chunks, LANES), jnp.float32),
        name="take_rows",
    )(rows, half, volume)


def fill_padded(plain_ref, index, base_ref, diff_ref, ahead, scale=None):
    chunks = plain_ref.shape[1]
    rows = base_ref.shape[1]
    value = plain_ref[index]
    if scale is not None:
        value = value * scale
    base_ref[index, pl.ds(0, 8), :] = jnp.zeros((8, LANES), jnp.float32)
    base_ref[index, pl.ds(8, 8), :] = jnp.zeros((8, LANES), jnp.float32)
    base_ref[index, pl.ds(1, chunks), :] = value
    padded = base_ref[index]
    lane = lax.broadcasted_iota(jnp.int32, (rows, LANES), 1)
    if ahead:
        turned = pltpu.roll(padded, LANES - 1, 1)
        carried = pltpu.roll(turned, rows - 1, 0)
        near = jnp.where(lane == LANES - 1, carried, turned)
    else:
        turned = pltpu.roll(padded, 1, 1)
        carried = pltpu.roll(turned, 1, 0)
        near = jnp.where(lane == 0, carried, turned)
    diff_ref[index] = near - padded


def shifted(base_ref, diff_ref, index, first, turn, lane_from, fraction):
    low = base_ref[index, pl.ds(first, 8), :]
    high = base_ref[index, pl.ds(first + 1, 8), :]
    low_diff = diff_ref[index, pl.ds(first, 8), :]
    high_diff = diff_ref[index, pl.ds(first + 1, 8), :]
    value = jnp.where(lane_from, low, high)
    diff = jnp.where(lane_from, low_diff, high_diff)
    return pltpu.roll(value + fraction * diff, turn, 1)


def split(offset):
    negative = (offset < 0).astype(jnp.int32)
    count = offset + LANES * negative
    return 1 - negative, count, jnp.where(count == 0, 0, LANES - count)


def project_kernel(angles_ref, first_ref, planes_ref, out_ref, base_ref, diff_ref):
    views = out_ref.shape[0]
    total = planes_ref.shape[0]
    lane = lax.broadcasted_iota(jnp.int32, (8, LANES), 1)

    def fill(layer, carry):
        fill_padded(planes_ref, layer, base_ref, diff_ref, True)
        return carry

    lax.fori_loop(0, total, fill, 0, unroll=4)

    group = 16

    def one_view(view, carry):
        slope = 2 * angles_ref[view] - ANGLES

        def layers(step, sums):
            sums = list(sums)
            for item in range(group):
                layer = step * group + item
                depth = first_ref[0] + 8 * (layer // 4) + item % 4
                product = depth * slope
                whole = lax.shift_right_arithmetic(product, 9)
                part = (product - whole * ANGLES).astype(jnp.float32) * (1.0 / ANGLES)
                first, count, turn = split(whole)
                sums[item % 4] = sums[item % 4] + shifted(
                    base_ref, diff_ref, layer, first, turn, lane >= count, part
                )
            return tuple(sums)

        zero = jnp.zeros((8, LANES), jnp.float32)
        sums = lax.fori_loop(0, total // group, layers, (zero,) * 4)
        ratio = jnp.full((8, LANES), slope, jnp.int32).astype(jnp.float32) / ANGLES
        weight = jnp.sqrt(1.0 + ratio * ratio)
        out_ref[view] = weight * ((sums[0] + sums[1]) + (sums[2] + sums[3]))
        return carry

    lax.fori_loop(0, views, one_view, 0)


def project(planes, angles, first_depth):
    total, chunks, _ = planes.shape
    views = angles.shape[0]
    return pl.pallas_call(
        project_kernel,
        in_specs=[
            pl.BlockSpec(memory_space=SMEM),
            pl.BlockSpec(memory_space=SMEM),
            pl.BlockSpec(memory_space=VMEM),
        ],
        out_specs=pl.BlockSpec(memory_space=VMEM),
        out_shape=jax.ShapeDtypeStruct((views, chunks, LANES), jnp.float32),
        scratch_shapes=[VMEM((total, 16, LANES), jnp.float32)] * 2,
        name="project",
    )(angles, first_depth, planes)


def backproject_kernel(
    scale, angles_ref, first_ref, rows_ref, out_ref, base_ref, diff_ref
):
    slabs, height = out_ref.shape[0], out_ref.shape[1]
    views = angles_ref.shape[0]
    lane = lax.broadcasted_iota(jnp.int32, (8, LANES), 1)

    def fill(view, carry):
        slope = 2 * angles_ref[view] - ANGLES
        ratio = jnp.full((8, LANES), slope, jnp.int32).astype(jnp.float32) / ANGLES
        weight = jnp.sqrt(1.0 + ratio * ratio) * scale
        for row in range(height):
            fill_padded(rows_ref, view * height + row, base_ref, diff_ref, False, weight)
        return carry

    lax.fori_loop(0, views, fill, 0)

    group = 4

    def one_slab(slab, carry):
        depth = first_ref[0] + 8 * slab

        def some_views(step, sums):
            sums = list(sums)
            for item in range(group):
                view = step * group + item
                product = depth * (2 * angles_ref[view] - ANGLES)
                whole = lax.shift_right_arithmetic(product, 9)
                part = (product - whole * ANGLES).astype(jnp.float32) * (1.0 / ANGLES)
                first, count, turn = split(-whole)
                for row in range(height):
                    sums[row] = sums[row] + shifted(
                        base_ref, diff_ref, view * height + row, first, turn, lane >= count, part
                    )
            return tuple(sums)

        zero = jnp.zeros((8, LANES), jnp.float32)
        sums = lax.fori_loop(0, views // group, some_views, (zero,) * height)
        for row in range(height):
            out_ref[slab, row] = sums[row]
        return carry

    lax.fori_loop(0, slabs, one_slab, 0)


def backproject(rows, angles, first_depth, slabs, scale):
    views, height, chunks, _ = rows.shape
    return pl.pallas_call(
        functools.partial(backproject_kernel, scale),
        in_specs=[
            pl.BlockSpec(memory_space=SMEM),
            pl.BlockSpec(memory_space=SMEM),
            pl.BlockSpec(memory_space=VMEM),
        ],
        out_specs=pl.BlockSpec(memory_space=VMEM),
        out_shape=jax.ShapeDtypeStruct((slabs, height, chunks, LANES), jnp.float32),
        scratch_shapes=[VMEM((views * height, 16, LANES), jnp.float32)] * 2,
        name="backproject",
    )(angles, first_depth, rows.reshape(views * height, chunks, LANES))


def place_kernel(rows_ref, value_ref, out_ref):
    count = value_ref.shape[0]

    def one(row, carry):
        out_ref[rows_ref[row]] = value_ref[row]
        return carry

    lax.fori_loop(0, count, one, 0, unroll=8)


def place(value, rows):
    return pl.pallas_call(
        place_kernel,
        in_specs=[pl.BlockSpec(memory_space=SMEM), pl.BlockSpec(memory_space=VMEM)],
        out_specs=pl.BlockSpec(memory_space=VMEM),
        out_shape=jax.ShapeDtypeStruct(value.shape, jnp.float32),
        name="place",
    )(rows, value)


def swap(value, axis):
    return lax.all_to_all(value, axis, 0, 0, tiled=True)


def to_all(value, axis):
    return swap(jnp.broadcast_to(value, (lax.axis_size(axis), *value.shape)), axis)


def per_device(volume, angle_index, detector_rows, measured):
    layers, row_count, columns = volume.shape
    slabs = lax.axis_size("gz")
    groups = lax.axis_size("vert")
    own_views, height, _ = measured.shape
    chunks = columns // LANES
    depth = layers * slabs
    views = own_views * groups
    vert = lax.axis_index("vert")
    own_row, half = vert // 2, vert % 2
    angles = to_all(angle_index, "vert").reshape(views)

    wanted = lax.dynamic_index_in_dim(
        detector_rows.reshape(slabs, height), own_row, 1, keepdims=False
    )
    sent = take_rows(volume, wanted, half.reshape(1))
    planes = swap(sent, "gz").reshape(slabs * layers // 2, chunks, LANES)
    first = (half * (layers // 2) - depth // 2).reshape(1)
    partial = project(planes, angles, first)
    parts = swap(partial.reshape(groups, own_views, chunks, LANES), "vert")
    parts = parts.reshape(height, 2, own_views, chunks, LANES)
    summed = jnp.transpose(parts[:, 0] + parts[:, 1], (1, 0, 2, 3))
    rays = measured.reshape(own_views, height, chunks, LANES)
    own = (summed - rays) * depth ** (-0.5)
    residual = own.reshape(own_views, height, columns)

    full = to_all(own, "vert").reshape(views, height, chunks, LANES)
    first_back = (vert - depth // 2).reshape(1)
    contrib = backproject(full, angles, first_back, slabs, views ** (-0.5))
    layer = swap(contrib, "gz").reshape(row_count, chunks, LANES)
    ordered = place(layer, detector_rows)
    block = swap(ordered.reshape(groups, row_count // groups, chunks, LANES), "vert")
    gradient = block.reshape(layers, row_count // groups, columns)
    return (residual, gradient)


def solution(mesh):
    in_specs = (P("gz", None, None), P("vert"), P(), P("vert", "gz", None))
    out_specs = (P("vert", "gz", None), P("gz", "vert", None))
    return jax.shard_map(
        per_device, mesh=mesh, in_specs=in_specs, out_specs=out_specs, check_vma=False
    )
```

```python
import functools

import jax
import jax.numpy as jnp
from jax import lax
from jax.experimental import pallas as pl
from jax.experimental.pallas import tpu as pltpu
from jax.sharding import PartitionSpec as P

ANGLES = 512
LANES = 128
VMEM = pltpu.VMEM
SMEM = pltpu.SMEM
LIMIT = 24 * 1024 * 1024
VIEWS_AT_ONCE = 2
SLABS_AT_ONCE = 2


def take_rows_kernel(rows_ref, layer_ref, slab_ref, out_ref):
    count, chunks, _ = out_ref.shape
    place = lax.broadcasted_iota(jnp.int32, (chunks, LANES), 0)

    def one(item, carry):
        row = rows_ref[item]
        start = pl.multiple_of(row // 8 * 8, 8)
        inside = row - start
        found = None
        for chunk in range(chunks):
            tile = slab_ref[0, pl.ds(start, 8), pl.ds(chunk * LANES, LANES)]
            turned = pltpu.roll(tile, (chunk + 8 - inside) % 8, 0)
            found = turned if found is None else jnp.where(place == chunk, turned, found)
        out_ref[item] = found
        return carry

    lax.fori_loop(0, count, one, 0, unroll=16)


def take_rows(volume, rows, layer):
    _, row_count, columns = volume.shape
    chunks = columns // LANES
    return pl.pallas_call(
        take_rows_kernel,
        grid_spec=pltpu.PrefetchScalarGridSpec(
            num_scalar_prefetch=2,
            grid=(1,),
            in_specs=[
                pl.BlockSpec(
                    (1, row_count, columns), lambda step, rows_ref, layer_ref: (layer_ref[0], 0, 0)
                )
            ],
            out_specs=pl.BlockSpec(
                (row_count, chunks, LANES), lambda step, rows_ref, layer_ref: (0, 0, 0)
            ),
        ),
        out_shape=jax.ShapeDtypeStruct((row_count, chunks, LANES), jnp.float32),
        name="take_rows",
    )(rows, layer, volume)


def fill_padded(value, index, base_ref, diff_ref, ahead):
    zero = jnp.zeros((8, LANES), jnp.float32)
    base_ref[index, pl.ds(0, 8), :] = zero
    base_ref[index, pl.ds(8, 8), :] = zero
    base_ref[index, pl.ds(1, 8), :] = value
    padded = base_ref[index]
    rows = padded.shape[0]
    lane = lax.broadcasted_iota(jnp.int32, (rows, LANES), 1)
    if ahead:
        turned = pltpu.roll(padded, LANES - 1, 1)
        carried = pltpu.roll(turned, rows - 1, 0)
        near = jnp.where(lane == LANES - 1, carried, turned)
    else:
        turned = pltpu.roll(padded, 1, 1)
        carried = pltpu.roll(turned, 1, 0)
        near = jnp.where(lane == 0, carried, turned)
    diff_ref[index] = (near - padded) * (1.0 / ANGLES)


def shifted(base_ref, diff_ref, height, index, offset, part, lane):
    first = 1 + lax.shift_right_arithmetic(offset, 7)
    count = lax.bitwise_and(offset, LANES - 1)
    turn = lax.bitwise_and(LANES - count, LANES - 1)
    keep = lane >= count
    fraction = part.astype(jnp.float32)
    found = []
    for row in range(height):
        slot = index * height + row
        value = jnp.where(
            keep, base_ref[slot, pl.ds(first, 8), :], base_ref[slot, pl.ds(first + 1, 8), :]
        )
        diff = jnp.where(
            keep, diff_ref[slot, pl.ds(first, 8), :], diff_ref[slot, pl.ds(first + 1, 8), :]
        )
        found.append(pltpu.roll(value + fraction * diff, turn, 1))
    return found


def weight_of(slope):
    ratio = jnp.full((8, LANES), slope, jnp.int32).astype(jnp.float32) / ANGLES
    return jnp.sqrt(1.0 + ratio * ratio)


def project_kernel(angles_ref, first_ref, planes_ref, out_ref, base_ref, diff_ref):
    views, height = out_ref.shape[0], out_ref.shape[1]
    slabs = planes_ref.shape[0]
    lane = lax.broadcasted_iota(jnp.int32, (8, LANES), 1)

    def fill(slab, carry):
        for row in range(height):
            fill_padded(planes_ref[slab, row], slab * height + row, base_ref, diff_ref, True)
        return carry

    lax.fori_loop(0, slabs, fill, 0, unroll=4)

    def some_views(step, carry):
        for item in range(VIEWS_AT_ONCE):
            view = step * VIEWS_AT_ONCE + item
            slope = 2 * angles_ref[view] - ANGLES
            sums = [None] * height
            for slab in range(slabs):
                product = (first_ref[0] + 8 * slab) * slope
                moved = shifted(
                    base_ref,
                    diff_ref,
                    height,
                    slab,
                    lax.shift_right_arithmetic(product, 9),
                    lax.bitwise_and(product, ANGLES - 1),
                    lane,
                )
                sums = moved if slab == 0 else [a + b for a, b in zip(sums, moved)]
            weight = weight_of(slope)
            for row in range(height):
                out_ref[view, row] = weight * sums[row]
        return carry

    lax.fori_loop(0, views // VIEWS_AT_ONCE, some_views, 0)


def padded_call(kernel, shape, name, angles, first, rows):
    items, height, chunks, _ = rows.shape
    return pl.pallas_call(
        kernel,
        in_specs=[
            pl.BlockSpec(memory_space=SMEM),
            pl.BlockSpec(memory_space=SMEM),
            pl.BlockSpec(memory_space=VMEM),
        ],
        out_specs=pl.BlockSpec(memory_space=VMEM),
        out_shape=jax.ShapeDtypeStruct(shape, jnp.float32),
        scratch_shapes=[VMEM((items * height, 16, LANES), jnp.float32)] * 2,
        compiler_params=pltpu.CompilerParams(vmem_limit_bytes=LIMIT),
        name=name,
    )(angles, first, rows)


def backproject_kernel(
    scale, angles_ref, first_ref, rows_ref, out_ref, base_ref, diff_ref
):
    slabs, height = out_ref.shape[0], out_ref.shape[1]
    views = angles_ref.shape[0]
    lane = lax.broadcasted_iota(jnp.int32, (8, LANES), 1)

    def fill(view, carry):
        weight = weight_of(2 * angles_ref[view] - ANGLES) * scale
        for row in range(height):
            fill_padded(
                rows_ref[view, row] * weight, view * height + row, base_ref, diff_ref, False
            )
        return carry

    lax.fori_loop(0, views, fill, 0, unroll=4)

    def some_slabs(step, carry):
        for item in range(SLABS_AT_ONCE):
            slab = step * SLABS_AT_ONCE + item
            depth = first_ref[0] + 8 * slab
            sums = [None] * height
            for view in range(views):
                product = depth * (2 * angles_ref[view] - ANGLES)
                moved = shifted(
                    base_ref,
                    diff_ref,
                    height,
                    view,
                    -lax.shift_right_arithmetic(product, 9),
                    lax.bitwise_and(product, ANGLES - 1),
                    lane,
                )
                sums = moved if view == 0 else [a + b for a, b in zip(sums, moved)]
            for row in range(height):
                out_ref[slab, row] = sums[row]
        return carry

    lax.fori_loop(0, slabs // SLABS_AT_ONCE, some_slabs, 0)


def place_kernel(rows_ref, value_ref, out_ref):
    count = value_ref.shape[0]

    def one(row, carry):
        out_ref[rows_ref[row]] = value_ref[row]
        return carry

    lax.fori_loop(0, count, one, 0, unroll=8)


def place(value, rows):
    return pl.pallas_call(
        place_kernel,
        in_specs=[pl.BlockSpec(memory_space=SMEM), pl.BlockSpec(memory_space=VMEM)],
        out_specs=pl.BlockSpec(memory_space=VMEM),
        out_shape=jax.ShapeDtypeStruct(value.shape, jnp.float32),
        compiler_params=pltpu.CompilerParams(vmem_limit_bytes=LIMIT),
        name="place",
    )(rows, value)


def swap(value, axis):
    return lax.all_to_all(value, axis, 0, 0, tiled=True)


def to_all(value, axis):
    return swap(jnp.broadcast_to(value, (lax.axis_size(axis), *value.shape)), axis)


def per_device(volume, angle_index, detector_rows, measured):
    layers, row_count, columns = volume.shape
    slabs = lax.axis_size("gz")
    groups = lax.axis_size("vert")
    own_views, height, _ = measured.shape
    chunks = columns // LANES
    depth = layers * slabs
    views = own_views * groups
    vert = lax.axis_index("vert")
    first = (vert - depth // 2).reshape(1)
    angles = to_all(angle_index, "vert").reshape(views)

    sent = take_rows(volume, detector_rows, vert.reshape(1))
    planes = swap(sent.reshape(slabs, height, chunks, LANES), "gz")
    partial = padded_call(
        project_kernel, (views, height, chunks, LANES), "project", angles, first, planes
    )
    parts = swap(partial.reshape(groups, own_views, height, chunks, LANES), "vert")
    summed = jnp.sum(parts, axis=0)
    rays = measured.reshape(own_views, height, chunks, LANES)
    own = (summed - rays) * depth ** (-0.5)
    residual = own.reshape(own_views, height, columns)

    full = to_all(own, "vert").reshape(views, height, chunks, LANES)
    contrib = padded_call(
        functools.partial(backproject_kernel, views ** (-0.5)),
        (slabs, height, chunks, LANES),
        "backproject",
        angles,
        first,
        full,
    )
    layer = swap(contrib, "gz").reshape(row_count, chunks, LANES)
    ordered = place(layer, detector_rows)
    block = swap(ordered.reshape(groups, row_count // groups, chunks, LANES), "vert")
    gradient = block.reshape(layers, row_count // groups, columns)
    return (residual, gradient)


def solution(mesh):
    in_specs = (P("gz", None, None), P("vert"), P(), P("vert", "gz", None))
    out_specs = (P("vert", "gz", None), P("gz", "vert", None))
    return jax.shard_map(
        per_device, mesh=mesh, in_specs=in_specs, out_specs=out_specs, check_vma=False
    )
```

```python
import functools

import jax
import jax.numpy as jnp
from jax import lax
from jax.experimental import pallas as pl
from jax.experimental.pallas import tpu as pltpu
from jax.sharding import PartitionSpec as P

ANGLES = 512
LANES = 128
VMEM = pltpu.VMEM
SMEM = pltpu.SMEM
LIMIT = 24 * 1024 * 1024
VIEWS_AT_ONCE = 2
SLABS_AT_ONCE = 2


def take_rows_kernel(rows_ref, layer_ref, volume_ref, out_ref, slab_ref, sems):
    count, chunks, _ = out_ref.shape
    copies = [
        pltpu.make_async_copy(
            volume_ref.at[layer_ref[0], :, pl.ds(chunk * LANES, LANES)],
            slab_ref.at[pl.ds(chunk * count, count), :],
            sems.at[chunk],
        )
        for chunk in range(chunks)
    ]
    for copy in copies:
        copy.start()
    for copy in copies:
        copy.wait()

    def one(item, carry):
        out_ref[item] = slab_ref[pl.ds(rows_ref[item], chunks, stride=count), :]
        return carry

    lax.fori_loop(0, count, one, 0, unroll=16)


def take_rows(volume, rows, layer):
    _, row_count, columns = volume.shape
    chunks = columns // LANES
    return pl.pallas_call(
        take_rows_kernel,
        in_specs=[
            pl.BlockSpec(memory_space=SMEM),
            pl.BlockSpec(memory_space=SMEM),
            pl.BlockSpec(memory_space=pl.ANY),
        ],
        out_specs=pl.BlockSpec(memory_space=VMEM),
        out_shape=jax.ShapeDtypeStruct((row_count, chunks, LANES), jnp.float32),
        scratch_shapes=[
            VMEM((row_count * chunks, LANES), jnp.float32),
            pltpu.SemaphoreType.DMA((chunks,)),
        ],
        name="take_rows",
    )(rows, layer, volume)


def fill_padded(value, index, base_ref, diff_ref, ahead):
    zero = jnp.zeros((8, LANES), jnp.float32)
    base_ref[index, pl.ds(0, 8), :] = zero
    base_ref[index, pl.ds(8, 8), :] = zero
    base_ref[index, pl.ds(1, 8), :] = value
    padded = base_ref[index]
    rows = padded.shape[0]
    lane = lax.broadcasted_iota(jnp.int32, (rows, LANES), 1)
    if ahead:
        turned = pltpu.roll(padded, LANES - 1, 1)
        carried = pltpu.roll(turned, rows - 1, 0)
        near = jnp.where(lane == LANES - 1, carried, turned)
    else:
        turned = pltpu.roll(padded, 1, 1)
        carried = pltpu.roll(turned, 1, 0)
        near = jnp.where(lane == 0, carried, turned)
    diff_ref[index] = (near - padded) * (1.0 / ANGLES)


def shifted(base_ref, diff_ref, height, index, offset, part, lane):
    first = 1 + lax.shift_right_arithmetic(offset, 7)
    count = lax.bitwise_and(offset, LANES - 1)
    turn = lax.bitwise_and(LANES - count, LANES - 1)
    keep = lane >= count
    fraction = part.astype(jnp.float32)
    found = []
    for row in range(height):
        slot = index * height + row
        value = jnp.where(
            keep, base_ref[slot, pl.ds(first, 8), :], base_ref[slot, pl.ds(first + 1, 8), :]
        )
        diff = jnp.where(
            keep, diff_ref[slot, pl.ds(first, 8), :], diff_ref[slot, pl.ds(first + 1, 8), :]
        )
        found.append(pltpu.roll(value + fraction * diff, turn, 1))
    return found


def weight_of(slope):
    ratio = jnp.full((8, LANES), slope, jnp.int32).astype(jnp.float32) / ANGLES
    return jnp.sqrt(1.0 + ratio * ratio)


def project_kernel(
    own_views, total, angles_in_ref, vert_ref, planes_ref, out_ref, base_ref, diff_ref, angles_ref
):
    sorted_angles(vert_ref[0], own_views, angles_in_ref, angles_ref)
    first_depth = vert_ref[0] - total // 2
    views, height = out_ref.shape[0], out_ref.shape[1]
    slabs = planes_ref.shape[0]
    lane = lax.broadcasted_iota(jnp.int32, (8, LANES), 1)

    def fill(slab, carry):
        for row in range(height):
            fill_padded(planes_ref[slab, row], slab * height + row, base_ref, diff_ref, True)
        return carry

    lax.fori_loop(0, slabs, fill, 0, unroll=4)

    def some_views(step, carry):
        for item in range(VIEWS_AT_ONCE):
            view = step * VIEWS_AT_ONCE + item
            slope = 2 * angles_ref[view] - ANGLES
            sums = [None] * height
            for slab in range(slabs):
                product = (first_depth + 8 * slab) * slope
                moved = shifted(
                    base_ref,
                    diff_ref,
                    height,
                    slab,
                    lax.shift_right_arithmetic(product, 9),
                    lax.bitwise_and(product, ANGLES - 1),
                    lane,
                )
                sums = moved if slab == 0 else [a + b for a, b in zip(sums, moved)]
            weight = weight_of(slope)
            for row in range(height):
                out_ref[view, row] = weight * sums[row]
        return carry

    lax.fori_loop(0, views // VIEWS_AT_ONCE, some_views, 0)


def padded_call(kernel, shape, name, angles, vert, rows):
    items, height, chunks, _ = rows.shape
    return pl.pallas_call(
        kernel,
        in_specs=[
            pl.BlockSpec(memory_space=SMEM),
            pl.BlockSpec(memory_space=SMEM),
            pl.BlockSpec(memory_space=VMEM),
        ],
        out_specs=pl.BlockSpec(memory_space=VMEM),
        out_shape=jax.ShapeDtypeStruct(shape, jnp.float32),
        scratch_shapes=[VMEM((items * height, 16, LANES), jnp.float32)] * 2
        + [SMEM(angles.shape, jnp.int32)],
        compiler_params=pltpu.CompilerParams(vmem_limit_bytes=LIMIT),
        name=name,
    )(angles, vert, rows)


def backproject_kernel(
    scale,
    own_views,
    total,
    angles_in_ref,
    vert_ref,
    rows_ref,
    out_ref,
    base_ref,
    diff_ref,
    angles_ref,
):
    sorted_angles(vert_ref[0], own_views, angles_in_ref, angles_ref)
    first_depth = vert_ref[0] - total // 2
    slabs, height = out_ref.shape[0], out_ref.shape[1]
    views = angles_ref.shape[0]
    lane = lax.broadcasted_iota(jnp.int32, (8, LANES), 1)

    def fill(view, carry):
        weight = weight_of(2 * angles_ref[view] - ANGLES) * scale
        for row in range(height):
            fill_padded(
                rows_ref[view, row] * weight, view * height + row, base_ref, diff_ref, False
            )
        return carry

    lax.fori_loop(0, views, fill, 0, unroll=4)

    def some_slabs(step, carry):
        for item in range(SLABS_AT_ONCE):
            slab = step * SLABS_AT_ONCE + item
            depth = first_depth + 8 * slab
            sums = [None] * height
            for view in range(views):
                product = depth * (2 * angles_ref[view] - ANGLES)
                moved = shifted(
                    base_ref,
                    diff_ref,
                    height,
                    view,
                    -lax.shift_right_arithmetic(product, 9),
                    lax.bitwise_and(product, ANGLES - 1),
                    lane,
                )
                sums = moved if view == 0 else [a + b for a, b in zip(sums, moved)]
            for row in range(height):
                out_ref[slab, row] = sums[row]
        return carry

    lax.fori_loop(0, slabs // SLABS_AT_ONCE, some_slabs, 0)


def place_kernel(rows_ref, value_ref, out_ref):
    count = value_ref.shape[0]

    def one(row, carry):
        out_ref[rows_ref[row]] = value_ref[row]
        return carry

    lax.fori_loop(0, count, one, 0, unroll=8)


def place(value, rows):
    return pl.pallas_call(
        place_kernel,
        in_specs=[pl.BlockSpec(memory_space=SMEM), pl.BlockSpec(memory_space=VMEM)],
        out_specs=pl.BlockSpec(memory_space=VMEM),
        out_shape=jax.ShapeDtypeStruct(value.shape, jnp.float32),
        compiler_params=pltpu.CompilerParams(vmem_limit_bytes=LIMIT),
        name="place",
    )(rows, value)


def swap(value, axis):
    return lax.all_to_all(value, axis, 0, 0, tiled=True)


def ring(shift, flip):
    return [(i, (i // 2 + shift) % 4 * 2 + (i % 2) ^ flip) for i in range(8)]


def angles_of_all(own):
    near = jnp.concatenate([own, lax.ppermute(own, "vert", ring(0, 1))])
    row = jnp.concatenate([near, lax.ppermute(near, "vert", ring(1, 0))])
    return jnp.concatenate([row, lax.ppermute(row, "vert", ring(2, 0))])


def sorted_angles(vert, own_views, angles_ref, table_ref):
    groups = angles_ref.shape[0] // own_views
    for block in range(groups):
        source_y = lax.rem(vert // 2 + 4 - block // 2, 4)
        source = 2 * source_y + lax.bitwise_xor(lax.rem(vert, 2), block % 2)
        for view in range(own_views):
            table_ref[source * own_views + view] = angles_ref[block * own_views + view]


def to_all(value, axis):
    return swap(jnp.broadcast_to(value, (lax.axis_size(axis), *value.shape)), axis)


def per_device(volume, angle_index, detector_rows, measured):
    layers, row_count, columns = volume.shape
    slabs = lax.axis_size("gz")
    groups = lax.axis_size("vert")
    own_views, height, _ = measured.shape
    chunks = columns // LANES
    depth = layers * slabs
    views = own_views * groups
    vert = lax.axis_index("vert").reshape(1)

    sent = take_rows(volume, detector_rows, vert)
    planes = swap(sent.reshape(slabs, height, chunks, LANES), "gz")
    angles = angles_of_all(angle_index)
    rays = measured.reshape(own_views, height, chunks, LANES)
    planes, rays = lax.optimization_barrier((planes, rays))
    partial = padded_call(
        functools.partial(project_kernel, own_views, depth),
        (views, height, chunks, LANES),
        "project",
        angles,
        vert,
        planes,
    )
    parts = swap(partial.reshape(groups, own_views, height, chunks, LANES), "vert")
    own = (jnp.sum(parts, axis=0) - rays) * depth ** (-0.5)

    full = to_all(own, "vert").reshape(views, height, chunks, LANES)
    contrib = padded_call(
        functools.partial(backproject_kernel, views ** (-0.5), own_views, depth),
        (slabs, height, chunks, LANES),
        "backproject",
        angles,
        vert,
        full,
    )
    layer = swap(contrib, "gz").reshape(row_count, chunks, LANES)
    ordered = place(layer, detector_rows)
    residual = own.reshape(own_views, height, columns)
    ordered, residual = lax.optimization_barrier((ordered, residual))
    block = swap(ordered.reshape(groups, row_count // groups, chunks, LANES), "vert")
    gradient = block.reshape(layers, row_count // groups, columns)
    return (residual, gradient)


def solution(mesh):
    in_specs = (P("gz", None, None), P("vert"), P(), P("vert", "gz", None))
    out_specs = (P("vert", "gz", None), P("gz", "vert", None))
    return jax.shard_map(
        per_device, mesh=mesh, in_specs=in_specs, out_specs=out_specs, check_vma=False
    )
```

```python
import functools

import jax
import jax.numpy as jnp
from jax import lax
from jax.experimental import pallas as pl
from jax.experimental.pallas import tpu as pltpu
from jax.sharding import PartitionSpec as P

ANGLES = 512
LANES = 128
VMEM = pltpu.VMEM
SMEM = pltpu.SMEM
LIMIT = 24 * 1024 * 1024
VIEWS_AT_ONCE = 8
SLABS_AT_ONCE = 8


def take_rows_kernel(rows_ref, volume_ref, out_ref, slab_ref, sems):
    count, chunks, _ = out_ref.shape
    layer = lax.axis_index("vert")
    copies = [
        pltpu.make_async_copy(
            volume_ref.at[layer, :, pl.ds(chunk * LANES, LANES)],
            slab_ref.at[pl.ds(chunk * count, count), :],
            sems.at[chunk],
        )
        for chunk in range(chunks)
    ]
    for copy in copies:
        copy.start()
    for copy in copies:
        copy.wait()

    def one(item, carry):
        out_ref[item] = slab_ref[pl.ds(rows_ref[item], chunks, stride=count), :]
        return carry

    lax.fori_loop(0, count, one, 0, unroll=16)


def take_rows(volume, rows):
    _, row_count, columns = volume.shape
    chunks = columns // LANES
    return pl.pallas_call(
        take_rows_kernel,
        in_specs=[
            pl.BlockSpec(memory_space=SMEM),
            pl.BlockSpec(memory_space=pl.ANY),
        ],
        out_specs=pl.BlockSpec(memory_space=VMEM),
        out_shape=jax.ShapeDtypeStruct((row_count, chunks, LANES), jnp.float32),
        scratch_shapes=[
            VMEM((row_count * chunks, LANES), jnp.float32),
            pltpu.SemaphoreType.DMA((chunks,)),
        ],
        name="take_rows",
    )(rows, volume)


def fill_padded(value, index, base_ref, diff_ref, ahead):
    zero = jnp.zeros((8, LANES), jnp.float32)
    base_ref[index, pl.ds(0, 8), :] = zero
    base_ref[index, pl.ds(8, 8), :] = zero
    base_ref[index, pl.ds(1, 8), :] = value
    padded = base_ref[index]
    rows = padded.shape[0]
    lane = lax.broadcasted_iota(jnp.int32, (rows, LANES), 1)
    if ahead:
        turned = pltpu.roll(padded, LANES - 1, 1)
        carried = pltpu.roll(turned, rows - 1, 0)
        near = jnp.where(lane == LANES - 1, carried, turned)
    else:
        turned = pltpu.roll(padded, 1, 1)
        carried = pltpu.roll(turned, 1, 0)
        near = jnp.where(lane == 0, carried, turned)
    diff_ref[index] = (near - padded) * (1.0 / ANGLES)


def shifted(base_ref, diff_ref, height, index, offset, part, lane):
    first = 1 + lax.shift_right_arithmetic(offset, 7)
    count = lax.bitwise_and(offset, LANES - 1)
    turn = lax.bitwise_and(LANES - count, LANES - 1)
    keep = lane >= count
    fraction = part.astype(jnp.float32)
    found = []
    for row in range(height):
        slot = index * height + row
        value = jnp.where(
            keep, base_ref[slot, pl.ds(first, 8), :], base_ref[slot, pl.ds(first + 1, 8), :]
        )
        diff = jnp.where(
            keep, diff_ref[slot, pl.ds(first, 8), :], diff_ref[slot, pl.ds(first + 1, 8), :]
        )
        found.append(pltpu.roll(value + fraction * diff, turn, 1))
    return found


def weight_of(slope):
    ratio = jnp.full((8, LANES), slope, jnp.int32).astype(jnp.float32) / ANGLES
    return jnp.sqrt(1.0 + ratio * ratio)


def project_kernel(
    own_views, total, angles_in_ref, planes_ref, out_ref, base_ref, diff_ref, angles_ref
):
    vert = lax.axis_index("vert")
    sorted_angles(vert, own_views, angles_in_ref, angles_ref)
    first_depth = vert - total // 2
    views, height = out_ref.shape[0], out_ref.shape[1]
    slabs = planes_ref.shape[0]
    lane = lax.broadcasted_iota(jnp.int32, (8, LANES), 1)

    def fill(slab, carry):
        for row in range(height):
            fill_padded(planes_ref[slab, row], slab * height + row, base_ref, diff_ref, True)
        return carry

    lax.fori_loop(0, slabs, fill, 0, unroll=4)

    def some_views(step, carry):
        for item in range(VIEWS_AT_ONCE):
            view = step * VIEWS_AT_ONCE + item
            slope = 2 * angles_ref[view] - ANGLES
            sums = [None] * height
            for slab in range(slabs):
                product = (first_depth + 8 * slab) * slope
                moved = shifted(
                    base_ref,
                    diff_ref,
                    height,
                    slab,
                    lax.shift_right_arithmetic(product, 9),
                    lax.bitwise_and(product, ANGLES - 1),
                    lane,
                )
                sums = moved if slab == 0 else [a + b for a, b in zip(sums, moved)]
            weight = weight_of(slope)
            for row in range(height):
                out_ref[view, row] = weight * sums[row]
        return carry

    lax.fori_loop(0, views // VIEWS_AT_ONCE, some_views, 0)


def padded_call(kernel, shapes, name, angles, rows, *more):
    items, height, chunks, _ = rows.shape
    whole = pl.BlockSpec(memory_space=VMEM)
    return pl.pallas_call(
        kernel,
        in_specs=[pl.BlockSpec(memory_space=SMEM)] + [whole] * (1 + len(more)),
        out_specs=[whole] * len(shapes),
        out_shape=[jax.ShapeDtypeStruct(shape, jnp.float32) for shape in shapes],
        scratch_shapes=[VMEM((items * height, 16, LANES), jnp.float32)] * 2
        + [SMEM(angles.shape, jnp.int32)],
        compiler_params=pltpu.CompilerParams(vmem_limit_bytes=LIMIT),
        name=name,
    )(angles, rows, *more)


def backproject_kernel(
    scale,
    own_views,
    total,
    angles_in_ref,
    rows_ref,
    own_ref,
    out_ref,
    residual_ref,
    base_ref,
    diff_ref,
    angles_ref,
):
    vert = lax.axis_index("vert")
    sorted_angles(vert, own_views, angles_in_ref, angles_ref)
    first_depth = vert - total // 2
    slabs, height = out_ref.shape[0], out_ref.shape[1]
    views = angles_ref.shape[0]
    lane = lax.broadcasted_iota(jnp.int32, (8, LANES), 1)

    def fill(view, carry):
        weight = weight_of(2 * angles_ref[view] - ANGLES) * scale
        for row in range(height):
            fill_padded(
                rows_ref[view, row] * weight, view * height + row, base_ref, diff_ref, False
            )
        return carry

    lax.fori_loop(0, views, fill, 0, unroll=4)

    def some_slabs(step, carry):
        for item in range(SLABS_AT_ONCE):
            slab = step * SLABS_AT_ONCE + item
            depth = first_depth + 8 * slab
            sums = [None] * height
            for view in range(views):
                product = depth * (2 * angles_ref[view] - ANGLES)
                moved = shifted(
                    base_ref,
                    diff_ref,
                    height,
                    view,
                    -lax.shift_right_arithmetic(product, 9),
                    lax.bitwise_and(product, ANGLES - 1),
                    lane,
                )
                sums = moved if view == 0 else [a + b for a, b in zip(sums, moved)]
            for row in range(height):
                out_ref[slab, row] = sums[row]
        return carry

    lax.fori_loop(0, slabs // SLABS_AT_ONCE, some_slabs, 0)
    for view in range(own_views):
        for chunk in range(own_ref.shape[2]):
            residual_ref[view, :, pl.ds(chunk * LANES, LANES)] = own_ref[view, :, chunk, :]


def place_kernel(rows_ref, value_ref, out_ref, sorted_ref):
    count, chunks, _ = value_ref.shape

    def one(row, carry):
        start = pl.multiple_of(rows_ref[row] * chunks, chunks)
        sorted_ref[pl.ds(start, chunks), :] = value_ref[row]
        return carry

    lax.fori_loop(0, count, one, 0, unroll=16)

    def eight(step, carry):
        for chunk in range(chunks):
            out_ref[pl.ds(pl.multiple_of(step * 8, 8), 8), pl.ds(chunk * LANES, LANES)] = (
                sorted_ref[pl.ds(step * 8 * chunks + chunk, 8, stride=chunks), :]
            )
        return carry

    lax.fori_loop(0, count // 8, eight, 0, unroll=4)


def place(value, rows):
    count, chunks, _ = value.shape
    return pl.pallas_call(
        place_kernel,
        in_specs=[pl.BlockSpec(memory_space=SMEM), pl.BlockSpec(memory_space=VMEM)],
        out_specs=pl.BlockSpec(memory_space=VMEM),
        out_shape=jax.ShapeDtypeStruct((count, chunks * LANES), jnp.float32),
        scratch_shapes=[VMEM((count * chunks, LANES), jnp.float32)],
        compiler_params=pltpu.CompilerParams(vmem_limit_bytes=LIMIT),
        name="place",
    )(rows, value)


def swap(value, axis):
    return lax.all_to_all(value, axis, 0, 0, tiled=True)


def ring(shift, flip):
    return [(i, (i // 2 + shift) % 4 * 2 + (i % 2) ^ flip) for i in range(8)]


def angles_of_all(own):
    near = jnp.concatenate([own, lax.ppermute(own, "vert", ring(0, 1))])
    row = jnp.concatenate([near, lax.ppermute(near, "vert", ring(1, 0))])
    return jnp.concatenate([row, lax.ppermute(row, "vert", ring(2, 0))])


def sorted_angles(vert, own_views, angles_ref, table_ref):
    groups = angles_ref.shape[0] // own_views
    for block in range(groups):
        source_y = lax.rem(vert // 2 + 4 - block // 2, 4)
        source = 2 * source_y + lax.bitwise_xor(lax.rem(vert, 2), block % 2)
        for view in range(own_views):
            table_ref[source * own_views + view] = angles_ref[block * own_views + view]


def to_all(value, axis):
    return swap(jnp.broadcast_to(value, (lax.axis_size(axis), *value.shape)), axis)


def per_device(volume, angle_index, detector_rows, measured):
    layers, row_count, columns = volume.shape
    slabs = lax.axis_size("gz")
    groups = lax.axis_size("vert")
    own_views, height, _ = measured.shape
    chunks = columns // LANES
    depth = layers * slabs
    views = own_views * groups

    sent = take_rows(volume, detector_rows)
    planes = swap(sent.reshape(slabs, height, chunks, LANES), "gz")
    angles = angles_of_all(angle_index)
    rays = measured.reshape(own_views, height, chunks, LANES)
    planes, rays = lax.optimization_barrier((planes, rays))
    (partial,) = padded_call(
        functools.partial(project_kernel, own_views, depth),
        [(views, height, chunks, LANES)],
        "project",
        angles,
        planes,
    )
    parts = swap(partial.reshape(groups, own_views, height, chunks, LANES), "vert")
    own = (jnp.sum(parts, axis=0) - rays) * depth ** (-0.5)

    full = to_all(own, "vert").reshape(views, height, chunks, LANES)
    contrib, residual = padded_call(
        functools.partial(backproject_kernel, views ** (-0.5), own_views, depth),
        [(slabs, height, chunks, LANES), (own_views, height, columns)],
        "backproject",
        angles,
        full,
        own,
    )
    layer = swap(contrib, "gz").reshape(row_count, chunks, LANES)
    ordered = place(layer, detector_rows)
    gradient = swap(ordered.reshape(groups, row_count // groups, columns), "vert")
    return (residual, gradient)


def solution(mesh):
    in_specs = (P("gz", None, None), P("vert"), P(), P("vert", "gz", None))
    out_specs = (P("vert", "gz", None), P("gz", "vert", None))
    return jax.shard_map(
        per_device, mesh=mesh, in_specs=in_specs, out_specs=out_specs, check_vma=False
    )
```

```python
import functools

import jax
import jax.numpy as jnp
from jax import lax
from jax.experimental import pallas as pl
from jax.experimental.pallas import tpu as pltpu
from jax.sharding import PartitionSpec as P

ANGLES = 512
LANES = 128
VMEM = pltpu.VMEM
SMEM = pltpu.SMEM
LIMIT = 24 * 1024 * 1024
VIEWS_AT_ONCE = 2
SLABS_AT_ONCE = 8


def take_rows_kernel(rows_ref, volume_ref, out_ref, slab_ref, sems):
    peers, tile, _ = out_ref.shape
    _, count, columns = volume_ref.shape
    chunks = columns // LANES
    part = tile // chunks
    vert = lax.axis_index("vert")
    y, x = lax.div(vert, 2), lax.rem(vert, 2)
    height = count // peers
    copies = [
        pltpu.make_async_copy(
            volume_ref.at[x * part + layer, :, pl.ds(chunk * LANES, LANES)],
            slab_ref.at[pl.ds((chunk * part + layer) * count, count), :],
            sems.at[chunk * part + layer],
        )
        for layer in range(part)
        for chunk in range(chunks)
    ]
    for copy in copies:
        copy.start()
    for copy in copies:
        copy.wait()

    def one(peer, carry):
        row = rows_ref[height * peer + y]
        for eight in range(tile // 8):
            out_ref[peer, pl.ds(eight * 8, 8), :] = slab_ref[
                pl.ds(eight * 8 * count + row, 8, stride=count), :
            ]
        return carry

    lax.fori_loop(0, peers, one, 0, unroll=4)


def take_rows(volume, rows, peers):
    layers, row_count, columns = volume.shape
    tile = layers // 2 * columns // LANES
    return pl.pallas_call(
        take_rows_kernel,
        in_specs=[
            pl.BlockSpec(memory_space=SMEM),
            pl.BlockSpec(memory_space=pl.ANY),
        ],
        out_specs=pl.BlockSpec(memory_space=VMEM),
        out_shape=jax.ShapeDtypeStruct((peers, tile, LANES), jnp.float32),
        scratch_shapes=[
            VMEM((tile * row_count, LANES), jnp.float32),
            pltpu.SemaphoreType.DMA((tile,)),
        ],
        name="take_rows",
    )(rows, volume)


def fill_padded(value, index, base_ref, diff_ref, ahead):
    zero = jnp.zeros((8, LANES), jnp.float32)
    base_ref[index, pl.ds(0, 8), :] = zero
    base_ref[index, pl.ds(8, 8), :] = zero
    base_ref[index, pl.ds(1, 8), :] = value
    padded = base_ref[index]
    rows = padded.shape[0]
    lane = lax.broadcasted_iota(jnp.int32, (rows, LANES), 1)
    if ahead:
        turned = pltpu.roll(padded, LANES - 1, 1)
        carried = pltpu.roll(turned, rows - 1, 0)
        near = jnp.where(lane == LANES - 1, carried, turned)
    else:
        turned = pltpu.roll(padded, 1, 1)
        carried = pltpu.roll(turned, 1, 0)
        near = jnp.where(lane == 0, carried, turned)
    diff_ref[index] = (near - padded) * (1.0 / ANGLES)


def shifted(base_ref, diff_ref, height, index, offset, part, lane):
    first = 1 + lax.shift_right_arithmetic(offset, 7)
    count = lax.bitwise_and(offset, LANES - 1)
    turn = lax.bitwise_and(LANES - count, LANES - 1)
    keep = lane >= count
    fraction = part.astype(jnp.float32)
    found = []
    for row in range(height):
        slot = index * height + row
        value = jnp.where(
            keep, base_ref[slot, pl.ds(first, 8), :], base_ref[slot, pl.ds(first + 1, 8), :]
        )
        diff = jnp.where(
            keep, diff_ref[slot, pl.ds(first, 8), :], diff_ref[slot, pl.ds(first + 1, 8), :]
        )
        found.append(pltpu.roll(value + fraction * diff, turn, 1))
    return found


def weight_of(slope):
    ratio = jnp.full((8, LANES), slope, jnp.int32).astype(jnp.float32) / ANGLES
    return jnp.sqrt(1.0 + ratio * ratio)


def project_kernel(
    own_views, total, angles_in_ref, planes_ref, kept_ref, sent_ref, base_ref, diff_ref, angles_ref
):
    vert = lax.axis_index("vert")
    y, x = lax.div(vert, 2), lax.rem(vert, 2)
    sorted_angles(vert, own_views, angles_in_ref, angles_ref)
    groups, padded, _, _ = base_ref.shape
    chunks = padded - 2
    tile = planes_ref.shape[0] // (2 * groups)
    lane = lax.broadcasted_iota(jnp.int32, (8, LANES), 1)
    layer = lax.broadcasted_iota(jnp.int32, (8, LANES), 0)
    upper = layer >= 4
    zero = jnp.zeros((8, LANES), jnp.float32)

    def fill(group, carry):
        start = group * 2 * tile
        values = [zero]
        for chunk in range(chunks):
            low = planes_ref[pl.ds(start + 4 * chunk, 8), :]
            high = planes_ref[pl.ds(start + tile + 4 * chunk - 4, 8), :]
            values.append(jnp.where(upper, high, low))
        values.append(zero)
        turned = [pltpu.roll(value, LANES - 1, 1) for value in values[1:-1]] + [zero]
        turned = [zero] + turned
        for chunk in range(padded):
            after = turned[min(chunk + 1, padded - 1)]
            near = jnp.where(lane == LANES - 1, after, turned[chunk])
            base_ref[group, chunk] = values[chunk]
            diff_ref[group, chunk] = (near - values[chunk]) * (1.0 / ANGLES)
        return carry

    lax.fori_loop(0, groups, fill, 0, unroll=2)

    depths = 8 * lax.div(layer, 4) + lax.rem(layer, 4) + 4 * x - total // 2

    def one_view(view):
        slope = 2 * angles_ref[view] - ANGLES
        sums = [zero] * chunks
        for group in range(groups):
            product = (depths + 16 * group) * slope
            offset = lax.shift_right_arithmetic(product, 9)
            fraction = lax.bitwise_and(product, ANGLES - 1).astype(jnp.float32)
            source = lax.shift_right_arithmetic(offset, 7) + (
                lane < lax.bitwise_and(offset, LANES - 1)
            ).astype(jnp.int32)
            before, after = source < 0, source > 0
            lanes = lax.bitwise_and(lane + offset, LANES - 1)
            mixed = [
                base_ref[group, chunk] + fraction * diff_ref[group, chunk]
                for chunk in range(padded)
            ]
            for chunk in range(chunks):
                value = jnp.where(
                    before, mixed[chunk], jnp.where(after, mixed[chunk + 2], mixed[chunk + 1])
                )
                sums[chunk] = sums[chunk] + jnp.take_along_axis(value, lanes, axis=1)
        ratio = jnp.full((1, LANES), slope, jnp.int32).astype(jnp.float32) / ANGLES
        weight = jnp.sqrt(1.0 + ratio * ratio)
        return [weight * jnp.sum(value, axis=0, keepdims=True) for value in sums]

    for out_ref, column in ((kept_ref, x), (sent_ref, 1 - x)):

        def some_views(step, carry):
            for item in range(VIEWS_AT_ONCE):
                place = step * VIEWS_AT_ONCE + item
                source_y = lax.rem(y + 4 - lax.div(place, own_views), 4)
                view = (source_y * 2 + column) * own_views + lax.rem(place, own_views)
                for chunk, value in enumerate(one_view(view)):
                    out_ref[place, pl.ds(chunk, 1), :] = value
            return carry

        lax.fori_loop(0, out_ref.shape[0] // VIEWS_AT_ONCE, some_views, 0)


def project(planes, angles, own_views, total):
    peers, tile, _ = planes.shape
    views = angles.shape[0]
    chunks = tile // 4
    whole = pl.BlockSpec(memory_space=VMEM)
    half = jax.ShapeDtypeStruct((views // 2, chunks, LANES), jnp.float32)
    return pl.pallas_call(
        functools.partial(project_kernel, own_views, total),
        in_specs=[pl.BlockSpec(memory_space=SMEM), whole],
        out_specs=[whole, whole],
        out_shape=[half, half],
        scratch_shapes=[VMEM((peers // 2, chunks + 2, 8, LANES), jnp.float32)] * 2
        + [SMEM(angles.shape, jnp.int32)],
        compiler_params=pltpu.CompilerParams(vmem_limit_bytes=LIMIT),
        name="project",
    )(angles, planes.reshape(peers * tile, LANES))


def backproject_kernel(
    scale, own_views, total, angles_in_ref, rows_ref, out_ref, residual_ref, base_ref, diff_ref, angles_ref
):
    vert = lax.axis_index("vert")
    sorted_angles(vert, own_views, angles_in_ref, angles_ref)
    first_depth = vert - total // 2
    slabs, height = out_ref.shape[0], out_ref.shape[1]
    views = angles_ref.shape[0]
    lane = lax.broadcasted_iota(jnp.int32, (8, LANES), 1)

    def sent_by(group, row, item):
        y, x = lax.div(group, 2), lax.rem(group, 2)
        return ((row * 2 + x) * 4 + lax.rem(row + 4 - y, 4)) * own_views + item

    def fill(group, carry):
        for item in range(own_views):
            view = group * own_views + item
            weight = weight_of(2 * angles_ref[view] - ANGLES) * scale
            for row in range(height):
                fill_padded(
                    rows_ref[sent_by(group, row, item)] * weight,
                    view * height + row,
                    base_ref,
                    diff_ref,
                    False,
                )
        return carry

    lax.fori_loop(0, views // own_views, fill, 0)

    def some_slabs(step, carry):
        for item in range(SLABS_AT_ONCE):
            slab = step * SLABS_AT_ONCE + item
            depth = first_depth + 8 * slab
            sums = [None] * height
            for view in range(views):
                product = depth * (2 * angles_ref[view] - ANGLES)
                moved = shifted(
                    base_ref,
                    diff_ref,
                    height,
                    view,
                    -lax.shift_right_arithmetic(product, 9),
                    lax.bitwise_and(product, ANGLES - 1),
                    lane,
                )
                sums = moved if view == 0 else [a + b for a, b in zip(sums, moved)]
            for row in range(height):
                out_ref[slab, row] = sums[row]
        return carry

    lax.fori_loop(0, slabs // SLABS_AT_ONCE, some_slabs, 0)
    for item in range(own_views):
        for row in range(height):
            value = rows_ref[sent_by(vert, row, item)]
            for chunk in range(value.shape[0]):
                residual_ref[item, pl.ds(row, 1), pl.ds(chunk * LANES, LANES)] = value[
                    chunk : chunk + 1, :
                ]


def backproject(rows, angles, own_views, height, slabs, total, scale):
    count, chunks, _ = rows.shape
    whole = pl.BlockSpec(memory_space=VMEM)
    return pl.pallas_call(
        functools.partial(backproject_kernel, scale, own_views, total),
        in_specs=[pl.BlockSpec(memory_space=SMEM), whole],
        out_specs=[whole, whole],
        out_shape=[
            jax.ShapeDtypeStruct((slabs, height, chunks, LANES), jnp.float32),
            jax.ShapeDtypeStruct((own_views, height, chunks * LANES), jnp.float32),
        ],
        scratch_shapes=[VMEM((count, 16, LANES), jnp.float32)] * 2
        + [SMEM(angles.shape, jnp.int32)],
        compiler_params=pltpu.CompilerParams(vmem_limit_bytes=LIMIT),
        name="backproject",
    )(angles, rows)


def place_kernel(rows_ref, value_ref, out_ref, sorted_ref):
    count, chunks, _ = value_ref.shape

    def one(row, carry):
        start = pl.multiple_of(rows_ref[row] * chunks, chunks)
        sorted_ref[pl.ds(start, chunks), :] = value_ref[row]
        return carry

    lax.fori_loop(0, count, one, 0, unroll=16)

    def eight(step, carry):
        for chunk in range(chunks):
            out_ref[pl.ds(pl.multiple_of(step * 8, 8), 8), pl.ds(chunk * LANES, LANES)] = (
                sorted_ref[pl.ds(step * 8 * chunks + chunk, 8, stride=chunks), :]
            )
        return carry

    lax.fori_loop(0, count // 8, eight, 0, unroll=4)


def place(value, rows):
    count, chunks, _ = value.shape
    return pl.pallas_call(
        place_kernel,
        in_specs=[pl.BlockSpec(memory_space=SMEM), pl.BlockSpec(memory_space=VMEM)],
        out_specs=pl.BlockSpec(memory_space=VMEM),
        out_shape=jax.ShapeDtypeStruct((count, chunks * LANES), jnp.float32),
        scratch_shapes=[VMEM((count * chunks, LANES), jnp.float32)],
        compiler_params=pltpu.CompilerParams(vmem_limit_bytes=LIMIT),
        name="place",
    )(rows, value)


def swap(value, axis):
    return lax.all_to_all(value, axis, 0, 0, tiled=True)


def ring(shift, flip):
    return [(i, (i // 2 + shift) % 4 * 2 + (i % 2) ^ flip) for i in range(8)]


def angles_of_all(own):
    near = jnp.concatenate([own, lax.ppermute(own, "vert", ring(0, 1))])
    row = jnp.concatenate([near, lax.ppermute(near, "vert", ring(1, 0))])
    return jnp.concatenate([row, lax.ppermute(row, "vert", ring(2, 0))])


def sorted_angles(vert, own_views, angles_ref, table_ref):
    groups = angles_ref.shape[0] // own_views
    for block in range(groups):
        source_y = lax.rem(vert // 2 + 4 - block // 2, 4)
        source = 2 * source_y + lax.bitwise_xor(lax.rem(vert, 2), block % 2)
        for view in range(own_views):
            table_ref[source * own_views + view] = angles_ref[block * own_views + view]


def to_all(value, axis):
    return swap(jnp.broadcast_to(value, (lax.axis_size(axis), *value.shape)), axis)


def per_device(volume, angle_index, detector_rows, measured):
    layers, row_count, columns = volume.shape
    slabs = lax.axis_size("gz")
    groups = lax.axis_size("vert")
    own_views, height, _ = measured.shape
    chunks = columns // LANES
    depth = layers * slabs
    views = own_views * groups

    vert = lax.axis_index("vert")
    y = vert // 2
    sent = take_rows(volume, detector_rows, slabs)
    planes = swap(sent, "gz")
    angles = angles_of_all(angle_index)
    rays = jnp.take(measured, (y + jnp.arange(height)) % height, axis=1)
    rays = jnp.swapaxes(rays, 0, 1).reshape(height, own_views, chunks, LANES)
    rays = jnp.stack(
        [rays[0]] + [lax.ppermute(rays[d], "vert", ring(d, 0)) for d in range(1, height)]
    )
    planes, rays = lax.optimization_barrier((planes, rays))
    kept, moved = project(planes, angles, own_views, depth)
    summed = kept + lax.ppermute(moved, "vert", ring(0, 1))
    own = (summed - rays.reshape(summed.shape)) * depth ** (-0.5)

    full = to_all(own, "vert").reshape(views * height, chunks, LANES)
    contrib, residual = backproject(
        full, angles, own_views, height, slabs, depth, views ** (-0.5)
    )
    layer = swap(contrib, "gz").reshape(row_count, chunks, LANES)
    ordered = place(layer, detector_rows)
    gradient = swap(ordered.reshape(groups, row_count // groups, columns), "vert")
    return (residual, gradient)


def solution(mesh):
    in_specs = (P("gz", None, None), P("vert"), P(), P("vert", "gz", None))
    out_specs = (P("vert", "gz", None), P("gz", "vert", None))
    return jax.shard_map(
        per_device, mesh=mesh, in_specs=in_specs, out_specs=out_specs, check_vma=False
    )
```

```python
import functools

import jax
import jax.numpy as jnp
from jax import lax
from jax.experimental import pallas as pl
from jax.experimental.pallas import tpu as pltpu
from jax.sharding import PartitionSpec as P

ANGLES = 512
LANES = 128
VMEM = pltpu.VMEM
SMEM = pltpu.SMEM
LIMIT = 24 * 1024 * 1024
VIEWS_AT_ONCE = 4
SLABS_AT_ONCE = 8


def take_rows_kernel(rows_ref, volume_ref, out_ref, slab_ref, sems):
    peers, tile, _ = out_ref.shape
    _, count, columns = volume_ref.shape
    chunks = columns // LANES
    part = tile // chunks
    vert = lax.axis_index("vert")
    y, x = lax.div(vert, 2), lax.rem(vert, 2)
    height = count // peers
    copies = [
        pltpu.make_async_copy(
            volume_ref.at[x * part + layer, :, pl.ds(chunk * LANES, LANES)],
            slab_ref.at[pl.ds((chunk * part + layer) * count, count), :],
            sems.at[chunk * part + layer],
        )
        for chunk in range(chunks)
        for layer in range(part)
    ]
    for copy in copies:
        copy.start()
    for eight in range(tile // 8):
        for copy in copies[eight * 8 : eight * 8 + 8]:
            copy.wait()

        def one(peer, carry):
            row = rows_ref[height * peer + y]
            out_ref[peer, pl.ds(eight * 8, 8), :] = slab_ref[
                pl.ds(eight * 8 * count + row, 8, stride=count), :
            ]
            return carry

        lax.fori_loop(0, peers, one, 0, unroll=16)


def take_rows(volume, rows, peers):
    layers, row_count, columns = volume.shape
    tile = layers // 2 * columns // LANES
    return pl.pallas_call(
        take_rows_kernel,
        in_specs=[
            pl.BlockSpec(memory_space=SMEM),
            pl.BlockSpec(memory_space=pl.ANY),
        ],
        out_specs=pl.BlockSpec(memory_space=VMEM),
        out_shape=jax.ShapeDtypeStruct((peers, tile, LANES), jnp.float32),
        scratch_shapes=[
            VMEM((tile * row_count, LANES), jnp.float32),
            pltpu.SemaphoreType.DMA((tile,)),
        ],
        name="take_rows",
    )(rows, volume)


def fill_padded(value, index, base_ref, diff_ref, ahead):
    zero = jnp.zeros((8, LANES), jnp.float32)
    base_ref[index, pl.ds(0, 8), :] = zero
    base_ref[index, pl.ds(8, 8), :] = zero
    base_ref[index, pl.ds(1, 8), :] = value
    padded = base_ref[index]
    rows = padded.shape[0]
    lane = lax.broadcasted_iota(jnp.int32, (rows, LANES), 1)
    if ahead:
        turned = pltpu.roll(padded, LANES - 1, 1)
        carried = pltpu.roll(turned, rows - 1, 0)
        near = jnp.where(lane == LANES - 1, carried, turned)
    else:
        turned = pltpu.roll(padded, 1, 1)
        carried = pltpu.roll(turned, 1, 0)
        near = jnp.where(lane == 0, carried, turned)
    diff_ref[index] = (near - padded) * (1.0 / ANGLES)


def shifted(base_ref, diff_ref, height, index, offset, part, lane):
    first = 1 + lax.shift_right_arithmetic(offset, 7)
    count = lax.bitwise_and(offset, LANES - 1)
    turn = lax.bitwise_and(LANES - count, LANES - 1)
    keep = lane >= count
    fraction = part.astype(jnp.float32)
    found = []
    for row in range(height):
        slot = index * height + row
        value = jnp.where(
            keep, base_ref[slot, pl.ds(first, 8), :], base_ref[slot, pl.ds(first + 1, 8), :]
        )
        diff = jnp.where(
            keep, diff_ref[slot, pl.ds(first, 8), :], diff_ref[slot, pl.ds(first + 1, 8), :]
        )
        found.append(pltpu.roll(value + fraction * diff, turn, 1))
    return found


def weight_of(slope):
    ratio = jnp.full((8, LANES), slope, jnp.int32).astype(jnp.float32) / ANGLES
    return jnp.sqrt(1.0 + ratio * ratio)


def project_kernel(
    own_views, total, angles_in_ref, planes_ref, kept_ref, sent_ref, base_ref, diff_ref, angles_ref
):
    vert = lax.axis_index("vert")
    y, x = lax.div(vert, 2), lax.rem(vert, 2)
    sorted_angles(vert, own_views, angles_in_ref, angles_ref)
    groups, padded, _, _ = base_ref.shape
    chunks = padded - 2
    tile = planes_ref.shape[0] // (2 * groups)
    lane = lax.broadcasted_iota(jnp.int32, (8, LANES), 1)
    layer = lax.broadcasted_iota(jnp.int32, (8, LANES), 0)
    upper = layer >= 4
    zero = jnp.zeros((8, LANES), jnp.float32)

    def fill(group, carry):
        start = group * 2 * tile
        values = [zero]
        for chunk in range(chunks):
            low = planes_ref[pl.ds(start + 4 * chunk, 8), :]
            high = planes_ref[pl.ds(start + tile + 4 * chunk - 4, 8), :]
            values.append(jnp.where(upper, high, low))
        values.append(zero)
        turned = [pltpu.roll(value, LANES - 1, 1) for value in values[1:-1]] + [zero]
        turned = [zero] + turned
        for chunk in range(padded):
            after = turned[min(chunk + 1, padded - 1)]
            near = jnp.where(lane == LANES - 1, after, turned[chunk])
            base_ref[group, chunk] = values[chunk]
            diff_ref[group, chunk] = (near - values[chunk]) * (1.0 / ANGLES)
        return carry

    lax.fori_loop(0, groups, fill, 0, unroll=2)

    depths = 8 * lax.div(layer, 4) + lax.rem(layer, 4) + 4 * x - total // 2

    def one_view(view):
        slope = 2 * angles_ref[view] - ANGLES
        sums = [zero] * chunks
        rising, falling = (slope > 0).astype(jnp.int32), (slope < 0).astype(jnp.int32)
        for group in range(groups):
            product = (depths + 16 * group) * slope
            offset = lax.shift_right_arithmetic(product, 9)
            fraction = lax.bitwise_and(product, ANGLES - 1).astype(jnp.float32)
            negative = rising if 2 * group < groups else falling
            low = lane >= offset + LANES * negative
            lanes = lax.bitwise_and(lane + offset, LANES - 1)
            mixed = [
                base_ref[group, 1 - negative + chunk]
                + fraction * diff_ref[group, 1 - negative + chunk]
                for chunk in range(chunks + 1)
            ]
            for chunk in range(chunks):
                value = jnp.where(low, mixed[chunk], mixed[chunk + 1])
                sums[chunk] = sums[chunk] + jnp.take_along_axis(value, lanes, axis=1)
        ratio = jnp.full((1, LANES), slope, jnp.int32).astype(jnp.float32) / ANGLES
        weight = jnp.sqrt(1.0 + ratio * ratio)
        return [weight * jnp.sum(value, axis=0, keepdims=True) for value in sums]

    for out_ref, column in ((kept_ref, x), (sent_ref, 1 - x)):

        def some_views(step, carry):
            for item in range(VIEWS_AT_ONCE):
                place = step * VIEWS_AT_ONCE + item
                source_y = lax.rem(y + 4 - lax.div(place, own_views), 4)
                view = (source_y * 2 + column) * own_views + lax.rem(place, own_views)
                for chunk, value in enumerate(one_view(view)):
                    out_ref[place, pl.ds(chunk, 1), :] = value
            return carry

        lax.fori_loop(0, out_ref.shape[0] // VIEWS_AT_ONCE, some_views, 0)


def project(planes, angles, own_views, total):
    peers, tile, _ = planes.shape
    views = angles.shape[0]
    chunks = tile // 4
    whole = pl.BlockSpec(memory_space=VMEM)
    half = jax.ShapeDtypeStruct((views // 2, chunks, LANES), jnp.float32)
    return pl.pallas_call(
        functools.partial(project_kernel, own_views, total),
        in_specs=[pl.BlockSpec(memory_space=SMEM), whole],
        out_specs=[whole, whole],
        out_shape=[half, half],
        scratch_shapes=[VMEM((peers // 2, chunks + 2, 8, LANES), jnp.float32)] * 2
        + [SMEM(angles.shape, jnp.int32)],
        compiler_params=pltpu.CompilerParams(
            vmem_limit_bytes=LIMIT
        ),
        name="project",
    )(angles, planes.reshape(peers * tile, LANES))


def backproject_kernel(
    scale, own_views, total, angles_in_ref, rows_ref, out_ref, residual_ref, base_ref, diff_ref, angles_ref
):
    vert = lax.axis_index("vert")
    sorted_angles(vert, own_views, angles_in_ref, angles_ref)
    first_depth = vert - total // 2
    slabs, height = out_ref.shape[0], out_ref.shape[1]
    views = angles_ref.shape[0]
    lane = lax.broadcasted_iota(jnp.int32, (8, LANES), 1)

    def sent_by(group, row, item):
        y, x = lax.div(group, 2), lax.rem(group, 2)
        return ((row * 2 + x) * 4 + lax.rem(row + 4 - y, 4)) * own_views + item

    def fill(group, carry):
        for item in range(own_views):
            view = group * own_views + item
            weight = weight_of(2 * angles_ref[view] - ANGLES) * scale
            for row in range(height):
                fill_padded(
                    rows_ref[sent_by(group, row, item)] * weight,
                    view * height + row,
                    base_ref,
                    diff_ref,
                    False,
                )
        return carry

    lax.fori_loop(0, views // own_views, fill, 0)

    def some_slabs(step, carry):
        for item in range(SLABS_AT_ONCE):
            slab = step * SLABS_AT_ONCE + item
            depth = first_depth + 8 * slab
            sums = [None] * height
            for view in range(views):
                product = depth * (2 * angles_ref[view] - ANGLES)
                moved = shifted(
                    base_ref,
                    diff_ref,
                    height,
                    view,
                    -lax.shift_right_arithmetic(product, 9),
                    lax.bitwise_and(product, ANGLES - 1),
                    lane,
                )
                sums = moved if view == 0 else [a + b for a, b in zip(sums, moved)]
            for row in range(height):
                out_ref[slab, row] = sums[row]
        return carry

    lax.fori_loop(0, slabs // SLABS_AT_ONCE, some_slabs, 0)
    for item in range(own_views):
        for row in range(height):
            value = rows_ref[sent_by(vert, row, item)]
            for chunk in range(value.shape[0]):
                residual_ref[item, pl.ds(row, 1), pl.ds(chunk * LANES, LANES)] = value[
                    chunk : chunk + 1, :
                ]


def backproject(rows, angles, own_views, height, slabs, total, scale):
    count, chunks, _ = rows.shape
    whole = pl.BlockSpec(memory_space=VMEM)
    return pl.pallas_call(
        functools.partial(backproject_kernel, scale, own_views, total),
        in_specs=[pl.BlockSpec(memory_space=SMEM), whole],
        out_specs=[whole, whole],
        out_shape=[
            jax.ShapeDtypeStruct((slabs, height, chunks, LANES), jnp.float32),
            jax.ShapeDtypeStruct((own_views, height, chunks * LANES), jnp.float32),
        ],
        scratch_shapes=[VMEM((count, 16, LANES), jnp.float32)] * 2
        + [SMEM(angles.shape, jnp.int32)],
        compiler_params=pltpu.CompilerParams(
            vmem_limit_bytes=LIMIT
        ),
        name="backproject",
    )(angles, rows)


def place_kernel(rows_ref, value_ref, out_ref, sorted_ref):
    count, chunks, _ = value_ref.shape

    def one(row, carry):
        start = pl.multiple_of(rows_ref[row] * chunks, chunks)
        sorted_ref[pl.ds(start, chunks), :] = value_ref[row]
        return carry

    lax.fori_loop(0, count, one, 0, unroll=16)

    def eight(step, carry):
        for chunk in range(chunks):
            out_ref[pl.ds(pl.multiple_of(step * 8, 8), 8), pl.ds(chunk * LANES, LANES)] = (
                sorted_ref[pl.ds(step * 8 * chunks + chunk, 8, stride=chunks), :]
            )
        return carry

    lax.fori_loop(0, count // 8, eight, 0, unroll=4)


def place(value, rows):
    count, chunks, _ = value.shape
    return pl.pallas_call(
        place_kernel,
        in_specs=[pl.BlockSpec(memory_space=SMEM), pl.BlockSpec(memory_space=VMEM)],
        out_specs=pl.BlockSpec(memory_space=VMEM),
        out_shape=jax.ShapeDtypeStruct((count, chunks * LANES), jnp.float32),
        scratch_shapes=[VMEM((count * chunks, LANES), jnp.float32)],
        compiler_params=pltpu.CompilerParams(vmem_limit_bytes=LIMIT),
        name="place",
    )(rows, value)


def swap(value, axis):
    return lax.all_to_all(value, axis, 0, 0, tiled=True)


def ring(shift, flip):
    return [(i, (i // 2 + shift) % 4 * 2 + (i % 2) ^ flip) for i in range(8)]


def sorted_angles(vert, own_views, angles_ref, table_ref):
    groups = angles_ref.shape[0] // own_views
    for block in range(groups):
        source_y = lax.rem(vert // 2 + 4 - block % 4, 4)
        source = 2 * source_y + lax.bitwise_xor(lax.rem(vert, 2), block // 4)
        for item in range(own_views):
            table_ref[source * own_views + item] = angles_ref[
                block * own_views + item
            ].astype(jnp.int32)


def to_all(value, axis):
    return swap(jnp.broadcast_to(value, (lax.axis_size(axis), *value.shape)), axis)


def per_device(volume, angle_index, detector_rows, measured):
    layers, row_count, columns = volume.shape
    slabs = lax.axis_size("gz")
    groups = lax.axis_size("vert")
    own_views, height, _ = measured.shape
    chunks = columns // LANES
    depth = layers * slabs
    views = own_views * groups

    vert = lax.axis_index("vert")
    y = vert // 2
    sent = take_rows(volume, detector_rows, slabs)
    planes = swap(sent, "gz")
    rays = jnp.take(measured, (y + jnp.arange(height)) % height, axis=1)
    rays = jnp.swapaxes(rays, 0, 1).reshape(height, own_views, chunks, LANES)
    note = jnp.pad(angle_index.astype(jnp.float32), (0, columns - own_views))
    note = jnp.broadcast_to(note.reshape(chunks, LANES), (height, 1, chunks, LANES))
    notes = jnp.concatenate([rays, note], axis=1)
    notes = jnp.stack(
        [notes[0]] + [lax.ppermute(notes[d], "vert", ring(d, 0)) for d in range(1, height)]
    )
    rays = notes[:, :own_views].reshape(views // 2, chunks, LANES)
    near = notes[:, own_views, 0, :own_views].reshape(views // 2)
    angles = jnp.concatenate([near, lax.ppermute(near, "vert", ring(0, 1))])
    planes, rays = lax.optimization_barrier((planes, rays))
    kept, moved = project(planes, angles, own_views, depth)
    summed = kept + lax.ppermute(moved, "vert", ring(0, 1))
    own = (summed - rays) * depth ** (-0.5)

    full = to_all(own, "vert").reshape(views * height, chunks, LANES)
    contrib, residual = backproject(
        full, angles, own_views, height, slabs, depth, views ** (-0.5)
    )
    layer = swap(contrib, "gz").reshape(row_count, chunks, LANES)
    ordered = place(layer, detector_rows)
    gradient = swap(ordered.reshape(groups, row_count // groups, columns), "vert")
    return (residual, gradient)


def solution(mesh):
    in_specs = (P("gz", None, None), P("vert"), P(), P("vert", "gz", None))
    out_specs = (P("vert", "gz", None), P("gz", "vert", None))
    return jax.shard_map(
        per_device, mesh=mesh, in_specs=in_specs, out_specs=out_specs, check_vma=False
    )
```

```python
import functools

import jax
import jax.numpy as jnp
from jax import lax
from jax.experimental import pallas as pl
from jax.experimental.pallas import tpu as pltpu
from jax.sharding import PartitionSpec as P

ANGLES = 512
LANES = 128
VMEM = pltpu.VMEM
SMEM = pltpu.SMEM
LIMIT = 24 * 1024 * 1024
VIEWS_AT_ONCE = 4
SLABS_AT_ONCE = 8


def take_rows_kernel(rows_ref, volume_ref, out_ref, slab_ref, sems):
    peers, tile, _ = out_ref.shape
    _, count, columns = volume_ref.shape
    chunks = columns // LANES
    part = tile // chunks
    vert = lax.axis_index("vert")
    y, x = lax.div(vert, 2), lax.rem(vert, 2)
    height = count // peers
    copies = [
        pltpu.make_async_copy(
            volume_ref.at[x * part + layer, :, pl.ds(chunk * LANES, LANES)],
            slab_ref.at[pl.ds((chunk * part + layer) * count, count), :],
            sems.at[chunk * part + layer],
        )
        for chunk in range(chunks)
        for layer in range(part)
    ]
    for copy in copies:
        copy.start()
    for eight in range(tile // 8):
        for copy in copies[eight * 8 : eight * 8 + 8]:
            copy.wait()

        def one(peer, carry):
            row = rows_ref[height * peer + y]
            out_ref[peer, pl.ds(eight * 8, 8), :] = slab_ref[
                pl.ds(eight * 8 * count + row, 8, stride=count), :
            ]
            return carry

        lax.fori_loop(0, peers, one, 0, unroll=16)


def take_rows(volume, rows, peers):
    layers, row_count, columns = volume.shape
    tile = layers // 2 * columns // LANES
    return pl.pallas_call(
        take_rows_kernel,
        in_specs=[
            pl.BlockSpec(memory_space=SMEM),
            pl.BlockSpec(memory_space=pl.ANY),
        ],
        out_specs=pl.BlockSpec(memory_space=VMEM),
        out_shape=jax.ShapeDtypeStruct((peers, tile, LANES), jnp.float32),
        scratch_shapes=[
            VMEM((tile * row_count, LANES), jnp.float32),
            pltpu.SemaphoreType.DMA((tile,)),
        ],
        name="take_rows",
    )(rows, volume)


def fill_padded(value, index, base_ref, diff_ref, ahead):
    zero = jnp.zeros((8, LANES), jnp.float32)
    base_ref[index, pl.ds(0, 8), :] = zero
    base_ref[index, pl.ds(8, 8), :] = zero
    base_ref[index, pl.ds(1, 8), :] = value
    padded = base_ref[index]
    rows = padded.shape[0]
    lane = lax.broadcasted_iota(jnp.int32, (rows, LANES), 1)
    if ahead:
        turned = pltpu.roll(padded, LANES - 1, 1)
        carried = pltpu.roll(turned, rows - 1, 0)
        near = jnp.where(lane == LANES - 1, carried, turned)
    else:
        turned = pltpu.roll(padded, 1, 1)
        carried = pltpu.roll(turned, 1, 0)
        near = jnp.where(lane == 0, carried, turned)
    diff_ref[index] = (near - padded) * (1.0 / ANGLES)


def shifted(base_ref, diff_ref, height, index, offset, part, lane):
    first = 1 + lax.shift_right_arithmetic(offset, 7)
    count = lax.bitwise_and(offset, LANES - 1)
    turn = lax.bitwise_and(LANES - count, LANES - 1)
    keep = lane >= count
    fraction = part.astype(jnp.float32)
    found = []
    for row in range(height):
        slot = index * height + row
        value = jnp.where(
            keep, base_ref[slot, pl.ds(first, 8), :], base_ref[slot, pl.ds(first + 1, 8), :]
        )
        diff = jnp.where(
            keep, diff_ref[slot, pl.ds(first, 8), :], diff_ref[slot, pl.ds(first + 1, 8), :]
        )
        found.append(pltpu.roll(value + fraction * diff, turn, 1))
    return found


def weight_of(slope):
    ratio = jnp.full((8, LANES), slope, jnp.int32).astype(jnp.float32) / ANGLES
    return jnp.sqrt(1.0 + ratio * ratio)


def project_kernel(
    own_views, total, other, angles_in_ref, planes_ref, out_ref, base_ref, diff_ref, angles_ref
):
    vert = lax.axis_index("vert")
    y, x = lax.div(vert, 2), lax.rem(vert, 2)
    sorted_angles(vert, own_views, angles_in_ref, angles_ref)
    groups, padded, _, _ = base_ref.shape
    chunks = padded - 2
    tile = planes_ref.shape[0] // (2 * groups)
    lane = lax.broadcasted_iota(jnp.int32, (8, LANES), 1)
    layer = lax.broadcasted_iota(jnp.int32, (8, LANES), 0)
    upper = layer >= 4
    zero = jnp.zeros((8, LANES), jnp.float32)

    def fill(group, carry):
        start = group * 2 * tile
        values = [zero]
        for chunk in range(chunks):
            low = planes_ref[pl.ds(start + 4 * chunk, 8), :]
            high = planes_ref[pl.ds(start + tile + 4 * chunk - 4, 8), :]
            values.append(jnp.where(upper, high, low))
        values.append(zero)
        turned = [pltpu.roll(value, LANES - 1, 1) for value in values[1:-1]] + [zero]
        turned = [zero] + turned
        for chunk in range(padded):
            after = turned[min(chunk + 1, padded - 1)]
            near = jnp.where(lane == LANES - 1, after, turned[chunk])
            base_ref[group, chunk] = values[chunk]
            diff_ref[group, chunk] = (near - values[chunk]) * (1.0 / ANGLES)
        return carry

    lax.fori_loop(0, groups, fill, 0, unroll=2)

    depths = 8 * lax.div(layer, 4) + lax.rem(layer, 4) + 4 * x - total // 2

    def one_view(view):
        slope = 2 * angles_ref[view] - ANGLES
        sums = [zero] * chunks
        rising, falling = (slope > 0).astype(jnp.int32), (slope < 0).astype(jnp.int32)
        for group in range(groups):
            product = (depths + 16 * group) * slope
            offset = lax.shift_right_arithmetic(product, 9)
            fraction = lax.bitwise_and(product, ANGLES - 1).astype(jnp.float32)
            negative = rising if 2 * group < groups else falling
            low = lane >= offset + LANES * negative
            lanes = lax.bitwise_and(lane + offset, LANES - 1)
            mixed = [
                base_ref[group, 1 - negative + chunk]
                + fraction * diff_ref[group, 1 - negative + chunk]
                for chunk in range(chunks + 1)
            ]
            for chunk in range(chunks):
                value = jnp.where(low, mixed[chunk], mixed[chunk + 1])
                sums[chunk] = sums[chunk] + jnp.take_along_axis(value, lanes, axis=1)
        ratio = jnp.full((1, LANES), slope, jnp.int32).astype(jnp.float32) / ANGLES
        weight = jnp.sqrt(1.0 + ratio * ratio)
        return [weight * jnp.sum(value, axis=0, keepdims=True) for value in sums]

    column = lax.bitwise_xor(x, other)

    def some_views(step, carry):
        for item in range(VIEWS_AT_ONCE):
            place = step * VIEWS_AT_ONCE + item
            source_y = lax.rem(y + 4 - lax.div(place, own_views), 4)
            view = (source_y * 2 + column) * own_views + lax.rem(place, own_views)
            for chunk, value in enumerate(one_view(view)):
                out_ref[place, pl.ds(chunk, 1), :] = value
        return carry

    lax.fori_loop(0, out_ref.shape[0] // VIEWS_AT_ONCE, some_views, 0)


def project(planes, angles, own_views, total, other):
    peers, tile, _ = planes.shape
    views = angles.shape[0]
    chunks = tile // 4
    whole = pl.BlockSpec(memory_space=VMEM)
    half = jax.ShapeDtypeStruct((views // 2, chunks, LANES), jnp.float32)
    return pl.pallas_call(
        functools.partial(project_kernel, own_views, total, other),
        in_specs=[pl.BlockSpec(memory_space=SMEM), whole],
        out_specs=whole,
        out_shape=half,
        scratch_shapes=[VMEM((peers // 2, chunks + 2, 8, LANES), jnp.float32)] * 2
        + [SMEM(angles.shape, jnp.int32)],
        compiler_params=pltpu.CompilerParams(
            vmem_limit_bytes=LIMIT
        ),
        cost_estimate=pl.CostEstimate(
            flops=20_000_000, bytes_accessed=1_000_000, transcendentals=0
        ),
        name="project",
    )(angles, planes.reshape(peers * tile, LANES))


def backproject_kernel(
    scale, own_views, total, angles_in_ref, rows_ref, out_ref, residual_ref, base_ref, diff_ref, angles_ref
):
    vert = lax.axis_index("vert")
    sorted_angles(vert, own_views, angles_in_ref, angles_ref)
    first_depth = vert - total // 2
    slabs, height = out_ref.shape[0], out_ref.shape[1]
    views = angles_ref.shape[0]
    lane = lax.broadcasted_iota(jnp.int32, (8, LANES), 1)

    def sent_by(group, row, item):
        y, x = lax.div(group, 2), lax.rem(group, 2)
        return ((row * 2 + x) * 4 + lax.rem(row + 4 - y, 4)) * own_views + item

    def fill(group, carry):
        for item in range(own_views):
            view = group * own_views + item
            weight = weight_of(2 * angles_ref[view] - ANGLES) * scale
            for row in range(height):
                fill_padded(
                    rows_ref[sent_by(group, row, item)] * weight,
                    view * height + row,
                    base_ref,
                    diff_ref,
                    False,
                )
        return carry

    lax.fori_loop(0, views // own_views, fill, 0)

    def some_slabs(step, carry):
        for item in range(SLABS_AT_ONCE):
            slab = step * SLABS_AT_ONCE + item
            depth = first_depth + 8 * slab
            sums = [None] * height
            for view in range(views):
                product = depth * (2 * angles_ref[view] - ANGLES)
                moved = shifted(
                    base_ref,
                    diff_ref,
                    height,
                    view,
                    -lax.shift_right_arithmetic(product, 9),
                    lax.bitwise_and(product, ANGLES - 1),
                    lane,
                )
                sums = moved if view == 0 else [a + b for a, b in zip(sums, moved)]
            for row in range(height):
                out_ref[slab, row] = sums[row]
        return carry

    lax.fori_loop(0, slabs // SLABS_AT_ONCE, some_slabs, 0)
    for item in range(own_views):
        for row in range(height):
            value = rows_ref[sent_by(vert, row, item)]
            for chunk in range(value.shape[0]):
                residual_ref[item, pl.ds(row, 1), pl.ds(chunk * LANES, LANES)] = value[
                    chunk : chunk + 1, :
                ]


def backproject(rows, angles, own_views, height, slabs, total, scale):
    count, chunks, _ = rows.shape
    whole = pl.BlockSpec(memory_space=VMEM)
    return pl.pallas_call(
        functools.partial(backproject_kernel, scale, own_views, total),
        in_specs=[pl.BlockSpec(memory_space=SMEM), whole],
        out_specs=[whole, whole],
        out_shape=[
            jax.ShapeDtypeStruct((slabs, height, chunks, LANES), jnp.float32),
            jax.ShapeDtypeStruct((own_views, height, chunks * LANES), jnp.float32),
        ],
        scratch_shapes=[VMEM((count, 16, LANES), jnp.float32)] * 2
        + [SMEM(angles.shape, jnp.int32)],
        compiler_params=pltpu.CompilerParams(
            vmem_limit_bytes=LIMIT
        ),
        name="backproject",
    )(angles, rows)


def place_kernel(rows_ref, value_ref, out_ref, sorted_ref):
    count, chunks, _ = value_ref.shape

    def one(row, carry):
        start = pl.multiple_of(rows_ref[row] * chunks, chunks)
        sorted_ref[pl.ds(start, chunks), :] = value_ref[row]
        return carry

    lax.fori_loop(0, count, one, 0, unroll=16)

    def eight(step, carry):
        for chunk in range(chunks):
            out_ref[pl.ds(pl.multiple_of(step * 8, 8), 8), pl.ds(chunk * LANES, LANES)] = (
                sorted_ref[pl.ds(step * 8 * chunks + chunk, 8, stride=chunks), :]
            )
        return carry

    lax.fori_loop(0, count // 8, eight, 0, unroll=4)


def place(value, rows):
    count, chunks, _ = value.shape
    return pl.pallas_call(
        place_kernel,
        in_specs=[pl.BlockSpec(memory_space=SMEM), pl.BlockSpec(memory_space=VMEM)],
        out_specs=pl.BlockSpec(memory_space=VMEM),
        out_shape=jax.ShapeDtypeStruct((count, chunks * LANES), jnp.float32),
        scratch_shapes=[VMEM((count * chunks, LANES), jnp.float32)],
        compiler_params=pltpu.CompilerParams(vmem_limit_bytes=LIMIT),
        name="place",
    )(rows, value)


def swap(value, axis):
    return lax.all_to_all(value, axis, 0, 0, tiled=True)


def ring(shift, flip):
    return [(i, (i // 2 + shift) % 4 * 2 + (i % 2) ^ flip) for i in range(8)]


def sorted_angles(vert, own_views, angles_ref, table_ref):
    groups = angles_ref.shape[0] // own_views
    for block in range(groups):
        source_y = lax.rem(vert // 2 + 4 - block % 4, 4)
        source = 2 * source_y + lax.bitwise_xor(lax.rem(vert, 2), block // 4)
        for item in range(own_views):
            table_ref[source * own_views + item] = angles_ref[
                block * own_views + item
            ].astype(jnp.int32)


def to_all(value, axis):
    return swap(jnp.broadcast_to(value, (lax.axis_size(axis), *value.shape)), axis)


def per_device(volume, angle_index, detector_rows, measured):
    layers, row_count, columns = volume.shape
    slabs = lax.axis_size("gz")
    groups = lax.axis_size("vert")
    own_views, height, _ = measured.shape
    chunks = columns // LANES
    depth = layers * slabs
    views = own_views * groups

    vert = lax.axis_index("vert")
    y = vert // 2
    sent = take_rows(volume, detector_rows, slabs)
    planes = swap(sent, "gz")
    rays = jnp.take(measured, (y + jnp.arange(height)) % height, axis=1)
    rays = jnp.swapaxes(rays, 0, 1).reshape(height, own_views, chunks, LANES)
    note = jnp.pad(angle_index.astype(jnp.float32), (0, columns - own_views))
    note = jnp.broadcast_to(note.reshape(chunks, LANES), (height, 1, chunks, LANES))
    notes = jnp.concatenate([rays, note], axis=1)
    notes = jnp.stack(
        [notes[0]] + [lax.ppermute(notes[d], "vert", ring(d, 0)) for d in range(1, height)]
    )
    rays = notes[:, :own_views].reshape(views // 2, chunks, LANES)
    near = notes[:, own_views, 0, :own_views].reshape(views // 2)
    angles = jnp.concatenate([near, lax.ppermute(near, "vert", ring(0, 1))])
    planes, rays = lax.optimization_barrier((planes, rays))
    moved = project(planes, angles, own_views, depth, 1)
    planes, moved = lax.optimization_barrier((planes, moved))
    kept = project(planes, angles, own_views, depth, 0)
    summed = kept + lax.ppermute(moved, "vert", ring(0, 1))
    own = (summed - rays) * depth ** (-0.5)

    full = to_all(own, "vert").reshape(views * height, chunks, LANES)
    contrib, residual = backproject(
        full, angles, own_views, height, slabs, depth, views ** (-0.5)
    )
    layer = swap(contrib, "gz").reshape(row_count, chunks, LANES)
    ordered = place(layer, detector_rows)
    gradient = swap(ordered.reshape(groups, row_count // groups, columns), "vert")
    return (residual, gradient)


def solution(mesh):
    in_specs = (P("gz", None, None), P("vert"), P(), P("vert", "gz", None))
    out_specs = (P("vert", "gz", None), P("gz", "vert", None))
    return jax.shard_map(
        per_device, mesh=mesh, in_specs=in_specs, out_specs=out_specs, check_vma=False
    )
```

```python
import functools

import jax
import jax.numpy as jnp
from jax import lax
from jax.experimental import pallas as pl
from jax.experimental.pallas import tpu as pltpu
from jax.sharding import PartitionSpec as P

ANGLES = 512
LANES = 128
VMEM = pltpu.VMEM
SMEM = pltpu.SMEM
LIMIT = 24 * 1024 * 1024
VIEWS_AT_ONCE = 4
SLABS_AT_ONCE = 8


def take_rows_kernel(rows_in_ref, volume_ref, out_ref, slab_ref, rows_ref, sems, rows_sem):
    peers, tile, _ = out_ref.shape
    _, count, columns = volume_ref.shape
    chunks = columns // LANES
    part = tile // chunks
    vert = lax.axis_index("vert")
    y, x = lax.div(vert, 2), lax.rem(vert, 2)
    height = count // peers
    copies = [
        pltpu.make_async_copy(
            volume_ref.at[x * part + layer, :, pl.ds(chunk * LANES, LANES)],
            slab_ref.at[pl.ds((chunk * part + layer) * count, count), :],
            sems.at[chunk * part + layer],
        )
        for chunk in range(chunks)
        for layer in range(part)
    ]
    table = pltpu.make_async_copy(rows_in_ref, rows_ref, rows_sem)
    table.start()
    for copy in copies:
        copy.start()
    table.wait()
    for eight in range(tile // 8):
        for copy in copies[eight * 8 : eight * 8 + 8]:
            copy.wait()

        def one(peer, carry):
            row = rows_ref[height * peer + y]
            out_ref[peer, pl.ds(eight * 8, 8), :] = slab_ref[
                pl.ds(eight * 8 * count + row, 8, stride=count), :
            ]
            return carry

        lax.fori_loop(0, peers, one, 0, unroll=16)


def take_rows(volume, rows, peers):
    layers, row_count, columns = volume.shape
    tile = layers // 2 * columns // LANES
    return pl.pallas_call(
        take_rows_kernel,
        in_specs=[pl.BlockSpec(memory_space=pl.ANY)] * 2,
        out_specs=pl.BlockSpec(memory_space=VMEM),
        out_shape=jax.ShapeDtypeStruct((peers, tile, LANES), jnp.float32),
        scratch_shapes=[
            VMEM(((tile + 1) * row_count, LANES), jnp.float32),
            SMEM((row_count,), jnp.int32),
            pltpu.SemaphoreType.DMA((tile,)),
            pltpu.SemaphoreType.DMA,
        ],
        name="take_rows",
    )(rows, volume)


def fill_padded(value, index, base_ref, diff_ref, ahead):
    zero = jnp.zeros((8, LANES), jnp.float32)
    base_ref[index, pl.ds(0, 8), :] = zero
    base_ref[index, pl.ds(8, 8), :] = zero
    base_ref[index, pl.ds(1, 8), :] = value
    padded = base_ref[index]
    rows = padded.shape[0]
    lane = lax.broadcasted_iota(jnp.int32, (rows, LANES), 1)
    if ahead:
        turned = pltpu.roll(padded, LANES - 1, 1)
        carried = pltpu.roll(turned, rows - 1, 0)
        near = jnp.where(lane == LANES - 1, carried, turned)
    else:
        turned = pltpu.roll(padded, 1, 1)
        carried = pltpu.roll(turned, 1, 0)
        near = jnp.where(lane == 0, carried, turned)
    diff_ref[index] = (near - padded) * (1.0 / ANGLES)


def shifted(base_ref, diff_ref, height, index, offset, part, lane):
    first = 1 + lax.shift_right_arithmetic(offset, 7)
    count = lax.bitwise_and(offset, LANES - 1)
    turn = lax.bitwise_and(LANES - count, LANES - 1)
    keep = lane >= count
    fraction = part.astype(jnp.float32)
    found = []
    for row in range(height):
        slot = index * height + row
        value = jnp.where(
            keep, base_ref[slot, pl.ds(first, 8), :], base_ref[slot, pl.ds(first + 1, 8), :]
        )
        diff = jnp.where(
            keep, diff_ref[slot, pl.ds(first, 8), :], diff_ref[slot, pl.ds(first + 1, 8), :]
        )
        found.append(pltpu.roll(value + fraction * diff, turn, 1))
    return found


def weight_of(slope):
    ratio = jnp.full((8, LANES), slope, jnp.int32).astype(jnp.float32) / ANGLES
    return jnp.sqrt(1.0 + ratio * ratio)


def project_kernel(
    own_views, total, other, angles_in_ref, planes_ref, out_ref, base_ref, diff_ref, angles_ref
):
    vert = lax.axis_index("vert")
    y, x = lax.div(vert, 2), lax.rem(vert, 2)
    sorted_angles(vert, own_views, angles_in_ref, angles_ref)
    groups, padded, _, _ = base_ref.shape
    chunks = padded - 2
    tile = planes_ref.shape[0] // (2 * groups)
    lane = lax.broadcasted_iota(jnp.int32, (8, LANES), 1)
    layer = lax.broadcasted_iota(jnp.int32, (8, LANES), 0)
    upper = layer >= 4
    zero = jnp.zeros((8, LANES), jnp.float32)

    def fill(group, carry):
        start = group * 2 * tile
        values = [zero]
        for chunk in range(chunks):
            low = planes_ref[pl.ds(start + 4 * chunk, 8), :]
            high = planes_ref[pl.ds(start + tile + 4 * chunk - 4, 8), :]
            values.append(jnp.where(upper, high, low))
        values.append(zero)
        turned = [pltpu.roll(value, LANES - 1, 1) for value in values[1:-1]] + [zero]
        turned = [zero] + turned
        for chunk in range(padded):
            after = turned[min(chunk + 1, padded - 1)]
            near = jnp.where(lane == LANES - 1, after, turned[chunk])
            base_ref[group, chunk] = values[chunk]
            diff_ref[group, chunk] = (near - values[chunk]) * (1.0 / ANGLES)
        return carry

    lax.fori_loop(0, groups, fill, 0, unroll=2)

    depths = 8 * lax.div(layer, 4) + lax.rem(layer, 4) + 4 * x - total // 2

    def one_view(view):
        slope = 2 * angles_ref[view] - ANGLES
        sums = [zero] * chunks
        rising, falling = (slope > 0).astype(jnp.int32), (slope < 0).astype(jnp.int32)
        for group in range(groups):
            product = (depths + 16 * group) * slope
            offset = lax.shift_right_arithmetic(product, 9)
            fraction = lax.bitwise_and(product, ANGLES - 1).astype(jnp.float32)
            negative = rising if 2 * group < groups else falling
            low = lane >= offset + LANES * negative
            lanes = lax.bitwise_and(lane + offset, LANES - 1)
            mixed = [
                base_ref[group, 1 - negative + chunk]
                + fraction * diff_ref[group, 1 - negative + chunk]
                for chunk in range(chunks + 1)
            ]
            for chunk in range(chunks):
                value = jnp.where(low, mixed[chunk], mixed[chunk + 1])
                sums[chunk] = sums[chunk] + jnp.take_along_axis(value, lanes, axis=1)
        ratio = jnp.full((1, LANES), slope, jnp.int32).astype(jnp.float32) / ANGLES
        weight = jnp.sqrt(1.0 + ratio * ratio)
        return [weight * jnp.sum(value, axis=0, keepdims=True) for value in sums]

    column = lax.bitwise_xor(x, other)

    def some_views(step, carry):
        for item in range(VIEWS_AT_ONCE):
            place = step * VIEWS_AT_ONCE + item
            source_y = lax.rem(y + 4 - lax.div(place, own_views), 4)
            view = (source_y * 2 + column) * own_views + lax.rem(place, own_views)
            for chunk, value in enumerate(one_view(view)):
                out_ref[place, pl.ds(chunk, 1), :] = value
        return carry

    lax.fori_loop(0, out_ref.shape[0] // VIEWS_AT_ONCE, some_views, 0)


def project(planes, angles, own_views, total, other):
    peers, tile, _ = planes.shape
    views = angles.shape[0]
    chunks = tile // 4
    whole = pl.BlockSpec(memory_space=VMEM)
    half = jax.ShapeDtypeStruct((views // 2, chunks, LANES), jnp.float32)
    return pl.pallas_call(
        functools.partial(project_kernel, own_views, total, other),
        in_specs=[pl.BlockSpec(memory_space=SMEM), whole],
        out_specs=whole,
        out_shape=half,
        scratch_shapes=[VMEM((peers // 2, chunks + 2, 8, LANES), jnp.float32)] * 2
        + [SMEM(angles.shape, jnp.int32)],
        compiler_params=pltpu.CompilerParams(
            vmem_limit_bytes=LIMIT
        ),
        cost_estimate=pl.CostEstimate(
            flops=20_000_000, bytes_accessed=1_000_000, transcendentals=0
        ),
        name="project",
    )(angles, planes.reshape(peers * tile, LANES))


def backproject_kernel(
    scale,
    own_views,
    total,
    angles_in_ref,
    rows_ref,
    out_ref,
    residual_out_ref,
    base_ref,
    diff_ref,
    angles_ref,
    residual_ref,
    sem,
):
    vert = lax.axis_index("vert")
    sorted_angles(vert, own_views, angles_in_ref, angles_ref)
    first_depth = vert - total // 2
    slabs, height = out_ref.shape[0], out_ref.shape[1]
    views = angles_ref.shape[0]
    lane = lax.broadcasted_iota(jnp.int32, (8, LANES), 1)

    def sent_by(group, row, item):
        y, x = lax.div(group, 2), lax.rem(group, 2)
        return ((row * 2 + x) * 4 + lax.rem(row + 4 - y, 4)) * own_views + item

    for item in range(own_views):
        for row in range(height):
            value = rows_ref[sent_by(vert, row, item)]
            for chunk in range(value.shape[0]):
                residual_ref[item, pl.ds(row, 1), pl.ds(chunk * LANES, LANES)] = value[
                    chunk : chunk + 1, :
                ]

    def fill(group, carry):
        for item in range(own_views):
            view = group * own_views + item
            weight = weight_of(2 * angles_ref[view] - ANGLES) * scale
            for row in range(height):
                fill_padded(
                    rows_ref[sent_by(group, row, item)] * weight,
                    view * height + row,
                    base_ref,
                    diff_ref,
                    False,
                )
        return carry

    lax.fori_loop(0, views // own_views, fill, 0)
    leaving = pltpu.make_async_copy(residual_ref, residual_out_ref, sem)
    leaving.start()

    def some_slabs(step, carry):
        for item in range(SLABS_AT_ONCE):
            slab = step * SLABS_AT_ONCE + item
            depth = first_depth + 8 * slab
            sums = [None] * height
            for view in range(views):
                product = depth * (2 * angles_ref[view] - ANGLES)
                moved = shifted(
                    base_ref,
                    diff_ref,
                    height,
                    view,
                    -lax.shift_right_arithmetic(product, 9),
                    lax.bitwise_and(product, ANGLES - 1),
                    lane,
                )
                sums = moved if view == 0 else [a + b for a, b in zip(sums, moved)]
            for row in range(height):
                out_ref[slab, row] = sums[row]
        return carry

    lax.fori_loop(0, slabs // SLABS_AT_ONCE, some_slabs, 0)
    leaving.wait()


def backproject(rows, angles, own_views, height, slabs, total, scale):
    count, chunks, _ = rows.shape
    whole = pl.BlockSpec(memory_space=VMEM)
    return pl.pallas_call(
        functools.partial(backproject_kernel, scale, own_views, total),
        in_specs=[pl.BlockSpec(memory_space=SMEM), whole],
        out_specs=[whole, pl.BlockSpec(memory_space=pltpu.HBM)],
        out_shape=[
            jax.ShapeDtypeStruct((slabs, height, chunks, LANES), jnp.float32),
            jax.ShapeDtypeStruct((own_views, height, chunks * LANES), jnp.float32),
        ],
        scratch_shapes=[VMEM((count, 16, LANES), jnp.float32)] * 2
        + [
            SMEM(angles.shape, jnp.int32),
            VMEM((own_views, height, chunks * LANES), jnp.float32),
            pltpu.SemaphoreType.DMA,
        ],
        compiler_params=pltpu.CompilerParams(
            vmem_limit_bytes=LIMIT
        ),
        name="backproject",
    )(angles, rows)


def place_kernel(rows_ref, value_ref, out_ref, sorted_ref):
    count, chunks, _ = value_ref.shape

    def one(row, carry):
        start = pl.multiple_of(rows_ref[row] * chunks, chunks)
        sorted_ref[pl.ds(start, chunks), :] = value_ref[row]
        return carry

    lax.fori_loop(0, count, one, 0, unroll=16)

    def eight(step, carry):
        for chunk in range(chunks):
            out_ref[pl.ds(pl.multiple_of(step * 8, 8), 8), pl.ds(chunk * LANES, LANES)] = (
                sorted_ref[pl.ds(step * 8 * chunks + chunk, 8, stride=chunks), :]
            )
        return carry

    lax.fori_loop(0, count // 8, eight, 0, unroll=4)


def place(value, rows):
    count, chunks, _ = value.shape
    return pl.pallas_call(
        place_kernel,
        in_specs=[pl.BlockSpec(memory_space=SMEM), pl.BlockSpec(memory_space=VMEM)],
        out_specs=pl.BlockSpec(memory_space=VMEM),
        out_shape=jax.ShapeDtypeStruct((count, chunks * LANES), jnp.float32),
        scratch_shapes=[VMEM(((count + 1) * chunks, LANES), jnp.float32)],
        compiler_params=pltpu.CompilerParams(vmem_limit_bytes=LIMIT),
        name="place",
    )(rows, value)


def swap(value, axis):
    return lax.all_to_all(value, axis, 0, 0, tiled=True)


def ring(shift, flip):
    return [(i, (i // 2 + shift) % 4 * 2 + (i % 2) ^ flip) for i in range(8)]


def sorted_angles(vert, own_views, angles_ref, table_ref):
    groups = angles_ref.shape[0] // own_views
    for block in range(groups):
        source_y = lax.rem(vert // 2 + 4 - block % 4, 4)
        source = 2 * source_y + lax.bitwise_xor(lax.rem(vert, 2), block // 4)
        for item in range(own_views):
            table_ref[source * own_views + item] = angles_ref[
                block * own_views + item
            ].astype(jnp.int32)


def to_all(value, axis):
    return swap(jnp.broadcast_to(value, (lax.axis_size(axis), *value.shape)), axis)


def per_device(volume, angle_index, detector_rows, measured):
    layers, row_count, columns = volume.shape
    slabs = lax.axis_size("gz")
    groups = lax.axis_size("vert")
    own_views, height, _ = measured.shape
    chunks = columns // LANES
    depth = layers * slabs
    views = own_views * groups

    vert = lax.axis_index("vert")
    y = vert // 2
    sent = take_rows(volume, detector_rows, slabs)
    planes = swap(sent, "gz")
    rays = jnp.take(measured, (y + jnp.arange(height)) % height, axis=1)
    rays = jnp.swapaxes(rays, 0, 1).reshape(height, own_views, chunks, LANES)
    note = jnp.pad(angle_index.astype(jnp.float32), (0, columns - own_views))
    note = jnp.broadcast_to(note.reshape(chunks, LANES), (height, 1, chunks, LANES))
    notes = jnp.concatenate([rays, note], axis=1)
    notes = jnp.stack(
        [notes[0]] + [lax.ppermute(notes[d], "vert", ring(d, 0)) for d in range(1, height)]
    )
    rays = notes[:, :own_views].reshape(views // 2, chunks, LANES)
    near = notes[:, own_views, 0, :own_views].reshape(views // 2)
    angles = jnp.concatenate([near, lax.ppermute(near, "vert", ring(0, 1))])
    planes, rays = lax.optimization_barrier((planes, rays))
    moved = project(planes, angles, own_views, depth, 1)
    planes, moved = lax.optimization_barrier((planes, moved))
    kept = project(planes, angles, own_views, depth, 0)
    summed = kept + lax.ppermute(moved, "vert", ring(0, 1))
    own = (summed - rays) * depth ** (-0.5)

    full = to_all(own, "vert").reshape(views * height, chunks, LANES)
    contrib, residual = backproject(
        full, angles, own_views, height, slabs, depth, views ** (-0.5)
    )
    layer = swap(contrib, "gz").reshape(row_count, chunks, LANES)
    ordered = place(layer, detector_rows)
    gradient = swap(ordered.reshape(groups, row_count // groups, columns), "vert")
    return (residual, gradient)


def solution(mesh):
    in_specs = (P("gz", None, None), P("vert"), P(), P("vert", "gz", None))
    out_specs = (P("vert", "gz", None), P("gz", "vert", None))
    return jax.shard_map(
        per_device, mesh=mesh, in_specs=in_specs, out_specs=out_specs, check_vma=False
    )
```
